128 devices in a mesh: seq: 16 (over z, x_lo, core), tp: 8 (over y, x_hi).
Axes of the slice: x: 4 (x_hi: 2, x_lo: 2; x = x_hi * 2 + x_lo), y: 4, z: 4, core: 2. Of those that a mesh axis runs over, the one named last changes fastest.
Arguments:
- hidden_in: bfloat16 [8192, 4608], P('seq'), may hold values from -6 to 6
- pre_gain: float32 [4608], replicated, may hold values from 0.5 to 1.5
- w_query: bfloat16 [4608, 4096], P(None, 'tp'), may hold values from -0.09375 to 0.09375
- key_cache: bfloat16 [16384, 2048], P('seq', 'tp'), may hold values from -12 to 12
- value_cache: bfloat16 [16384, 2048], P('seq', 'tp'), may hold values from -6 to 6
- w_out: bfloat16 [4096, 4608], P('tp'), may hold values from -0.75 to 0.75
- post_gain: float32 [4608], replicated, may hold values from 0.5 to 1.5
- starts: int32 [16], replicated, may hold values from 0 to 15872, as said below
- counts: int32 [16], replicated, may hold values from 512 to 1024, as said below
Outputs:
- layer_out: bfloat16 [8192, 4608], P(('seq', 'tp'))
The draws below stay inside these ranges and needn't reach their ends.
Inputs may be any that keep to these rules, and one draw needn't show every extreme that they name: The queries of shard s sit at positions starts[s] to starts[s] + 511, all inside the filled rows of shard s, that is from s * 1024 to s * 1024 + counts[s] - 1. `counts`: at least one shard is full.
All inputs are finite; a program needn't handle non-finite values.
Results may differ from the reference program's by a relative error of at most 0.012.
Values may be sent and summed in bfloat16 or wider, within the bound.
A program may use at most 128 MiB of HBM per device.

```python
import jax
import jax.numpy as jnp
from jax import lax

D = 4608
H = 32
KVH = 16
HD = 128
WINDOW = 4096
CTX_DEV = 1024
Q_DEV = 512
HALO = 4
CONTEXT = 16384
TOKENS = 8192
N_SEQ = 16
N_TP = 8


def fill_table(key):
    count_key = jax.random.fold_in(key, 11)
    full_key = jax.random.fold_in(key, 12)
    offset_key = jax.random.fold_in(key, 13)
    shard_ids = jnp.arange(N_SEQ, dtype=jnp.int32)
    counts = jax.random.randint(count_key, (N_SEQ,), Q_DEV, CTX_DEV + 1, dtype=jnp.int32)
    full_shard = jax.random.randint(full_key, (), 0, N_SEQ, dtype=jnp.int32)
    counts = jnp.where(shard_ids == full_shard, jnp.int32(CTX_DEV), counts)
    offsets = jax.random.randint(offset_key, (N_SEQ,), 0, counts - Q_DEV + 1, dtype=jnp.int32)
    starts = shard_ids * CTX_DEV + offsets
    return (starts.astype(jnp.int32), counts.astype(jnp.int32))


def draw_starts(key, part):
    return fill_table(key)[0]


def draw_counts(key, part):
    return fill_table(key)[1]


def levels(rng, shape, shards, least, top_value):
    def one(axis_at, blocks):
        draws = jax.random.uniform(jax.random.fold_in(jax.random.fold_in(rng, 6), axis_at), (blocks,), jnp.float32, least / len(shards), top_value / len(shards))
        return jnp.repeat(jnp.exp(draws), shape[axis_at] // blocks).reshape((-1,) + (1,) * (len(shape) - axis_at - 1))

    level = one(*shards[0])
    for cut in shards[1:]:
        level = level * one(*cut)
    return level


def gaussian(key, shape, scale, reach, shards=(), kind=jnp.bfloat16):
    gain = levels(key, shape, shards, -0.22, 0.18) if shards else 1.0
    result = jax.random.normal(key, shape, jnp.float32) * scale * gain
    return jnp.minimum(jnp.maximum(result, -reach), reach).astype(kind)


def setup_inputs(seed: int = 0) -> dict:
    seeds = jax.random.split(jax.random.key(seed), 10)
    hidden_in = gaussian(seeds[0], (TOKENS, D), 1.0, 6.0, ((0, 16),))
    pre_gain = jnp.clip(1.0 + 0.1 * jax.random.normal(seeds[1], (D,), jnp.float32), 0.5, 1.5)
    w_query = gaussian(seeds[2], (D, H * HD), D ** -0.5, 0.09375, ((1, 8),))
    key_cache = gaussian(seeds[3], (CONTEXT, KVH * HD), 2.0, 12.0, ((0, 16), (1, 8)))
    value_cache = gaussian(seeds[4], (CONTEXT, KVH * HD), 1.0, 6.0, ((0, 16), (1, 8)))
    w_out = gaussian(seeds[5], (H * HD, D), (H * HD // 64) ** -0.5, 0.75, ((0, 8),))
    post_gain = jnp.clip(1.0 + 0.1 * jax.random.normal(seeds[6], (D,), jnp.float32), 0.5, 1.5)
    starts = draw_starts(jax.random.fold_in(seeds[9], 71), 0)
    counts = draw_counts(jax.random.fold_in(seeds[9], 71), 0)
    return dict(hidden_in=hidden_in, pre_gain=pre_gain, w_query=w_query, key_cache=key_cache, value_cache=value_cache, w_out=w_out, post_gain=post_gain, starts=starts, counts=counts)


def reference(hidden_in, pre_gain, w_query, key_cache, value_cache, w_out, post_gain, starts, counts):
    per_group = H // KVH
    key_span = (HALO + 1) * CTX_DEV
    inputs = hidden_in.astype(jnp.float32)
    normed = (inputs * lax.rsqrt(lax.optimization_barrier(jnp.mean(inputs * inputs, axis=-1, keepdims=True)) + 0.1) * pre_gain).astype(jnp.bfloat16)
    queries = (jnp.dot(normed, w_query, preferred_element_type=jnp.float32) * (D // H) ** (-0.5)).astype(jnp.bfloat16)
    padding = jnp.zeros((HALO * CTX_DEV, KVH * HD), jnp.bfloat16)
    keys_padded = jnp.concatenate([padding, key_cache], axis=0)
    values_padded = jnp.concatenate([padding, value_cache], axis=0)
    w_groups = w_out.astype(jnp.float32).reshape(N_TP, H * HD // N_TP, D)

    def one_shard(shard):
        shard = shard.astype(jnp.int32)
        query_block = lax.dynamic_slice_in_dim(queries, (shard * Q_DEV).astype(jnp.int32), Q_DEV, 0)
        key_block = lax.dynamic_slice_in_dim(keys_padded, (shard * CTX_DEV).astype(jnp.int32), key_span, 0)
        value_block = lax.dynamic_slice_in_dim(values_padded, (shard * CTX_DEV).astype(jnp.int32), key_span, 0)
        key_pos = (shard - HALO) * CTX_DEV + jnp.arange(key_span, dtype=jnp.int32)
        source = jnp.clip(key_pos // CTX_DEV, 0, N_SEQ - 1).astype(jnp.int32)
        filled = (key_pos >= 0) & (key_pos - source * CTX_DEV < counts[source])
        query_pos = starts[shard] + jnp.arange(Q_DEV, dtype=jnp.int32)
        allowed = filled[None, :] & (key_pos[None, :] <= query_pos[:, None]) & (key_pos[None, :] > query_pos[:, None] - WINDOW)
        query_f = lax.optimization_barrier(query_block).astype(jnp.float32).reshape(Q_DEV, KVH, per_group, HD)
        key_f = key_block.astype(jnp.float32).reshape(key_span, KVH, HD)
        value_f = value_block.astype(jnp.float32).reshape(key_span, KVH, HD)
        scores = jnp.einsum('qkgd,ckd->kgqc', query_f, key_f, precision=lax.Precision.HIGHEST)
        scores = 50.0 * jnp.tanh(scores / 50.0)
        weight = jnp.where(allowed[None, None], jnp.exp(scores), jnp.float32(0.0))
        denominator = lax.optimization_barrier(jnp.sum(weight, axis=-1))
        weight16 = lax.optimization_barrier(weight.astype(jnp.bfloat16)).astype(jnp.float32)
        context = jnp.einsum('kgqc,ckd->qkgd', weight16, value_f, precision=lax.Precision.HIGHEST)
        attended = (context / jnp.transpose(denominator, (2, 0, 1))[..., None]).reshape(Q_DEV, H * HD).astype(jnp.bfloat16)
        attended_f = lax.optimization_barrier(attended).astype(jnp.float32).reshape(Q_DEV, N_TP, H * HD // N_TP)
        partial_value = jnp.einsum('qtf,tfd->tqd', attended_f, w_groups, precision=lax.Precision.HIGHEST)
        partial_value = lax.optimization_barrier(partial_value.astype(jnp.bfloat16)).astype(jnp.float32)
        projected = lax.optimization_barrier(jnp.sum(partial_value, axis=0))
        residual = lax.dynamic_slice_in_dim(hidden_in, (shard * Q_DEV).astype(jnp.int32), Q_DEV, 0).astype(jnp.float32)
        mixed = residual + projected * lax.rsqrt(lax.optimization_barrier(jnp.mean(projected * projected, axis=-1, keepdims=True)) + 0.1) * post_gain
        return mixed.astype(jnp.bfloat16)
    layer_out = lax.map(one_shard, jnp.arange(N_SEQ, dtype=jnp.int32))
    return layer_out.reshape(N_SEQ * Q_DEV, D)
```

```python
import math

import jax
import jax.numpy as jnp
from jax import lax
from jax.experimental import pallas as pl
from jax.experimental.pallas import tpu as pltpu
from jax.sharding import PartitionSpec as P

MESH = pl.DeviceIdType.MESH
D = 4608
HD = 128
CTX = 1024
QR = 512
HALO = 4
CH = 128
NCH = CTX // CH
GR = 256
WCH = 16
NW = 8
NP = 6
PC = D // NP
BF = jnp.bfloat16
F32 = jnp.float32
SCALE = 144 ** (-0.5)
EXP_SCALE = 50.0 * math.log2(math.e)
TO_Z, TO_X, TO_C1, TO_C3 = range(4)
SLOT = {TO_Z: 4, TO_X: 2, TO_C1: 1, TO_C3: 3}
PIECES = (0, 3, 1, 4, 2, 5)


def layer(
    gain, post, starts, counts, hid_in, wq_in, k_in, v_in, wo_in, out,
    hid, nrm, wq, kbuf, vbuf, qbuf, acc, att, attr, wo, wp, keep, rs_s, rs_r,
    hid_sem, load_sem, kv_s, kv_r, w_s, w_r, att_s, att_r, rss_sem, rsr_sem,
):
    s = lax.axis_index("seq")
    t = lax.axis_index("tp")
    c = s % 2
    xl = (s // 2) % 2
    z = s // 4
    xh = t % 2
    y = t // 2

    def dev(z_=None, xl_=None, c_=None, y_=None, xh_=None):
        z_ = z if z_ is None else z_
        xl_ = xl if xl_ is None else xl_
        c_ = c if c_ is None else c_
        y_ = y if y_ is None else y_
        xh_ = xh if xh_ is None else xh_
        return (z_ * 4 + xl_ * 2 + c_, y_ * 2 + xh_)

    z_up = dev(z_=(z + 1) % 4)
    z_down = dev(z_=(z + 3) % 4)
    x_near = dev(xl_=1 - xl)
    core = dev(c_=1 - c)
    x_far = dev(xh_=1 - xh)
    cross = dev(xl_=1 - xl, xh_=1 - xh)
    y_up = dev(y_=(y + 1) % 4)
    y_down = dev(y_=(y + 3) % 4)

    def block_row(slot_delta):
        return ((y + slot_delta) % 4) * 128

    loads = []
    for slot, delta in enumerate((3, 1, 2, 0)):
        rows = pl.ds(pl.multiple_of(block_row(delta), 128), 128)
        loads.append(
            pltpu.make_async_copy(hid_in.at[rows, :], hid.at[pl.ds(slot * 128, 128), :], hid_sem.at[slot])
        )
    load_wq = pltpu.make_async_copy(wq_in, wq, load_sem.at[0])
    load_k = pltpu.make_async_copy(k_in, kbuf.at[0], load_sem.at[1])
    load_v = pltpu.make_async_copy(v_in, vbuf.at[0], load_sem.at[2])
    load_wo = pltpu.make_async_copy(wo_in, wo, load_sem.at[3])
    for load in loads:
        load.start()
    load_wq.start()

    barrier = pltpu.get_barrier_semaphore()
    for other in (z_up, z_down, x_near, core, x_far, cross, y_up, y_down):
        pl.semaphore_signal(barrier, inc=1, device_id=other, device_id_type=MESH)
    pl.semaphore_wait(barrier, 8)

    def remote(src, dst, send, recv, to):
        return pltpu.make_async_remote_copy(
            src_ref=src, dst_ref=dst, send_sem=send, recv_sem=recv, device_id=to, device_id_type=MESH
        )

    kv_to = {TO_Z: z_up, TO_X: x_near, TO_C1: core, TO_C3: core}

    def kv_copies(stream, j, src):
        slot = SLOT[stream]
        rows = pl.ds(j * CH, CH)
        k_src = k_in.at[rows, :] if src is None else kbuf.at[src, rows, :]
        v_src = v_in.at[rows, :] if src is None else vbuf.at[src, rows, :]
        return (
            remote(k_src, kbuf.at[slot, rows, :], kv_s.at[stream, j, 0], kv_r.at[stream, j, 0], kv_to[stream]),
            remote(v_src, vbuf.at[slot, rows, :], kv_s.at[stream, j, 1], kv_r.at[stream, j, 1], kv_to[stream]),
        )

    def kv_send(stream, j, src):
        for copy in kv_copies(stream, j, src):
            copy.start()

    def kv_wait(stream, j):
        for copy in kv_copies(stream, j, SLOT[stream]):
            copy.wait_recv()

    parity = z % 2
    W_CROSS, W_DOWN, W_CA, W_CB = range(4)
    w_to = {W_CROSS: cross, W_DOWN: z_down, W_CA: core, W_CB: core}

    def w_copy(stream, j, quarter, from_input=False):
        rows = pl.ds(pl.multiple_of(quarter * 128 + j * WCH, WCH), WCH)
        src = wo_in.at[rows, :] if from_input else wp.at[rows, :]
        return remote(src, wp.at[rows, :], w_s.at[stream, j], w_r.at[stream, j], w_to[stream])

    mine = parity * 2 + c
    above = (1 - parity) * 2 + c
    w_arrives = {
        W_CROSS: mine,
        W_DOWN: above,
        W_CA: parity * 2 + (1 - c),
        W_CB: (1 - parity) * 2 + (1 - c),
    }

    for j in range(NCH):
        kv_send(TO_Z, j, None)

        @pl.when(xl == 0)
        def _():
            kv_send(TO_X, j, None)

        @pl.when(c == 0)
        def _():
            kv_send(TO_C1, j, None)

        w_copy(W_CROSS, j, mine, from_input=True).start()
    load_k.start()
    load_v.start()
    load_wo.start()

    def step_f(j):
        kv_wait(TO_Z, j)

        @pl.when(xl == 1)
        def _():
            kv_send(TO_X, j, 4)

        @pl.when(c == 1)
        def _():
            kv_send(TO_C3, j, 4)

    def step_g(j):
        kv_wait(TO_X, j)

        @pl.when(c == 0)
        def _():
            kv_send(TO_C3, j, 2)

        @pl.when(c == 1)
        def _():
            kv_send(TO_C1, j, 2)

    def step_e(j):
        kv_wait(TO_C1, j)
        kv_wait(TO_C3, j)

    def step_w(j):
        w_copy(W_CROSS, j, mine).wait_recv()
        w_copy(W_DOWN, j, mine).start()
        w_copy(W_CA, j, mine).start()

    def step_z(j):
        w_copy(W_DOWN, j, above).wait_recv()
        w_copy(W_CB, j, above).start()

    def norm_rows(i, carry):
        rows = pl.ds(pl.multiple_of(i * 16, 16), 16)
        x = hid[rows, :].astype(F32)
        r = lax.rsqrt(jnp.mean(x * x, axis=-1, keepdims=True) + 0.1)
        nrm[rows, :] = (x * r * gain[...]).astype(BF)
        return carry

    for slot in range(4):
        loads[slot].wait()
        lax.fori_loop(slot * 8, slot * 8 + 8, norm_rows, 0)
    step_f(0)
    step_w(0)
    load_wq.wait()
    for kh in range(2):
        q = jnp.dot(nrm[...], wq[:, kh * 256 : kh * 256 + 256], preferred_element_type=F32)
        q = (q * SCALE).astype(BF)
        for slot in range(4):
            for g in range(2):
                qbuf[kh, slot * 256 + g * 128 : slot * 256 + g * 128 + 128, :] = q[
                    slot * 128 : slot * 128 + 128, g * 128 : g * 128 + 128
                ]
    acc[...] = jnp.zeros_like(acc)

    off = starts[s] - s * CTX
    filled = {}
    for d in range(1, HALO + 1):
        source = s - d
        filled[d] = jnp.where(source >= 0, counts[jnp.maximum(source, 0)], 0)

    def attend(base, kh, tile):
        lanes = pl.ds(pl.multiple_of(kh * HD, HD), HD)
        rows = pl.ds(pl.multiple_of(tile * 512, 512), 512)
        q = qbuf[kh, rows, :]
        row_ids = lax.broadcasted_iota(jnp.int32, (GR, HD), 0)

        def scores(d):
            key = kbuf[d, base : base + GR, lanes]
            return lax.dot_general(q, key, (((1,), (1,)), ((), ())), preferred_element_type=F32)

        def weights(x):
            return jnp.exp2(jnp.tanh(x * (1.0 / 50.0)) * EXP_SCALE)

        def values(d):
            v = vbuf[d, base : base + GR, lanes]
            if d == 0:
                return jnp.concatenate([v, jnp.ones_like(v)], axis=1)
            keep_row = jnp.where(row_ids < filled[d] - base, 1.0, 0.0).astype(BF)
            return jnp.concatenate([v * keep_row, keep_row], axis=1)

        total = None
        for d in (1, 2, 3):
            w = weights(scores(d)).astype(BF)
            part = jnp.dot(w, values(d), preferred_element_type=F32)
            total = part if total is None else total + part
        near, far = scores(0), scores(4)
        pattern = lax.broadcasted_iota(jnp.int32, (128, GR), 1) - lax.broadcasted_iota(jnp.int32, (128, GR), 0)
        w_near, w_far = [], []
        for u in range(4):
            limit = off + block_row(3 - 2 * (u // 2) - tile) - base
            is_near = pattern <= limit
            part_rows = slice(u * 128, u * 128 + 128)
            w = weights(jnp.where(is_near, near[part_rows], far[part_rows]))
            w_near.append(jnp.where(is_near, w, 0.0).astype(BF))
            w_far.append(jnp.where(is_near, 0.0, w).astype(BF))
        total = total + jnp.dot(jnp.concatenate(w_near, axis=0), values(0), preferred_element_type=F32)
        total = total + jnp.dot(jnp.concatenate(w_far, axis=0), values(4), preferred_element_type=F32)
        acc[kh, rows, :] += total

    def attend_tiles(base, kh):
        def body(tile, carry):
            attend(base, kh, tile)
            return carry

        lax.fori_loop(0, 2, body, 0)

    step_f(1)
    step_w(1)
    step_g(0)
    step_f(2)
    step_w(2)
    load_k.wait()
    load_v.wait()
    step_g(1)
    step_e(0)
    step_e(1)
    attend_tiles(0, 0)
    step_f(3)
    step_w(3)
    step_z(0)
    attend_tiles(0, 1)
    step_f(4)
    step_w(4)
    step_z(1)
    step_g(2)
    step_f(5)
    step_w(5)
    step_g(3)
    step_e(2)
    step_e(3)
    attend_tiles(256, 0)
    step_f(6)
    step_w(6)
    step_z(2)
    attend_tiles(256, 1)
    step_g(4)
    step_f(7)
    step_w(7)
    step_z(3)
    step_z(4)
    step_g(5)
    step_e(4)
    step_e(5)
    attend_tiles(512, 0)
    step_g(6)
    step_z(5)
    attend_tiles(512, 1)
    step_g(7)
    step_e(6)
    step_e(7)

    def att_copy(slot):
        rows = pl.ds(pl.multiple_of((1 - xh) * 64, 64), 64)
        return remote(att.at[slot, rows, :], attr.at[slot], att_s.at[slot], att_r.at[slot], x_far)

    for tile in range(2):
        def body(kh, carry):
            attend(768, kh, tile)
            return carry

        lax.fori_loop(0, 2, body, 0)
        for kh in range(2):
            a = acc[kh, tile * 512 : tile * 512 + 512, :]
            o = (a[:, :HD] / a[:, HD:]).astype(BF)
            for u in range(4):
                head = kh * 2 + u % 2
                att[2 * tile + u // 2, :, head * HD : head * HD + HD] = o[u * 128 : u * 128 + 128, :]
        for slot in (2 * tile, 2 * tile + 1):
            att_copy(slot).start()
        step_z(6 + tile)

    for j in range(NW):
        w_copy(W_CA, j, w_arrives[W_CA]).wait_recv()
        w_copy(W_CB, j, w_arrives[W_CB]).wait_recv()
    load_wo.wait()

    def rs_copy(step, p):
        to = y_up if p < NP // 2 else y_down
        return remote(rs_s.at[step, p], rs_r.at[step, p], rss_sem.at[step, p], rsr_sem.at[step, p], to)

    own_rows = pl.ds(pl.multiple_of(xh * 64, 64), 64)
    for tile in range(2):
        for slot in (2 * tile, 2 * tile + 1):
            att_copy(slot).wait_recv()
        lhs = jnp.concatenate([att[2 * tile, own_rows, :], att[2 * tile + 1, own_rows, :]], axis=0)
        lhs_far = jnp.concatenate([attr[2 * tile], attr[2 * tile + 1]], axis=0)
        for p in PIECES:
            cols = slice(p * PC, p * PC + PC)
            r = jnp.dot(lhs, wo[:, cols], preferred_element_type=F32)
            r = r + jnp.dot(lhs_far, wp[:, cols], preferred_element_type=F32)
            if tile == 0:
                first, later = (r[:64], r[64:]) if p < NP // 2 else (r[64:], r[:64])
                rs_s[0, p] = first.astype(BF)
                rs_copy(0, p).start()
                keep[1, :, cols] = later
            else:
                keep[0, :, cols] = r[:64]
                keep[2, :, cols] = r[64:]
    for step in (1, 2):
        for p in PIECES:
            cols = slice(p * PC, p * PC + PC)
            rs_copy(step - 1, p).wait_recv()
            rs_s[step, p] = (rs_r[step - 1, p].astype(F32) + keep[step - 1, :, cols]).astype(BF)
            rs_copy(step, p).start()
    squares = jnp.zeros((64, 1), F32)
    for p in PIECES:
        cols = slice(p * PC, p * PC + PC)
        rs_copy(2, p).wait_recv()
        part = rs_r[2, p].astype(F32) + keep[2, :, cols]
        keep[2, :, cols] = part
        squares = squares + jnp.sum(part * part, axis=-1, keepdims=True)
    factor = lax.rsqrt(squares * (1.0 / D) + 0.1)
    residual_rows = pl.ds(pl.multiple_of(384 + xh * 64, 64), 64)
    for p in range(NP):
        cols = slice(p * PC, p * PC + PC)
        residual = hid[residual_rows, cols].astype(F32)
        out[:, cols] = (residual + keep[2, :, cols] * factor * post[:, cols]).astype(BF)

    for j in range(NCH):
        for stream in (TO_Z, TO_X, TO_C1, TO_C3):
            for copy in kv_copies(stream, j, SLOT[stream]):
                copy.wait_send()
    for j in range(NW):
        for stream in (W_CROSS, W_DOWN, W_CA, W_CB):
            w_copy(stream, j, mine).wait_send()
    for slot in range(4):
        att_copy(slot).wait_send()
    for step in range(3):
        for p in PIECES:
            rs_copy(step, p).wait_send()


def shards(hidden_in, pre_gain, w_query, key_cache, value_cache, w_out, post_gain, starts, counts):
    vmem = pl.BlockSpec(memory_space=pltpu.VMEM)
    smem = pl.BlockSpec(memory_space=pltpu.SMEM)
    hbm = pl.BlockSpec(memory_space=pl.ANY)
    dma = pltpu.SemaphoreType.DMA
    return pl.pallas_call(
        layer,
        out_shape=jax.ShapeDtypeStruct((64, D), BF),
        in_specs=[vmem, vmem, smem, smem, hbm, hbm, hbm, hbm, hbm],
        out_specs=vmem,
        scratch_shapes=[
            pltpu.VMEM((QR, D), BF),
            pltpu.VMEM((QR, D), BF),
            pltpu.VMEM((D, 512), BF),
            pltpu.VMEM((HALO + 1, CTX, 256), BF),
            pltpu.VMEM((HALO + 1, CTX, 256), BF),
            pltpu.VMEM((2, 1024, HD), BF),
            pltpu.VMEM((2, 1024, 256), F32),
            pltpu.VMEM((4, 128, 512), BF),
            pltpu.VMEM((4, 64, 512), BF),
            pltpu.VMEM((512, D), BF),
            pltpu.VMEM((512, D), BF),
            pltpu.VMEM((3, 64, D), F32),
            pltpu.VMEM((3, NP, 64, PC), BF),
            pltpu.VMEM((3, NP, 64, PC), BF),
            dma((4,)),
            dma((4,)),
            dma((4, NCH, 2)),
            dma((4, NCH, 2)),
            dma((4, NW)),
            dma((4, NW)),
            dma((4,)),
            dma((4,)),
            dma((3, NP)),
            dma((3, NP)),
        ],
        compiler_params=pltpu.CompilerParams(
            collective_id=0, has_side_effects=True, vmem_limit_bytes=60 * 1024 * 1024
        ),
        name="layer",
    )(
        pre_gain.reshape(1, D), post_gain.reshape(1, D), starts, counts,
        hidden_in, w_query, key_cache, value_cache, w_out,
    )


def solution(mesh):
    in_specs = (
        P("seq", None),
        P(),
        P(None, "tp"),
        P("seq", "tp"),
        P("seq", "tp"),
        P("tp", None),
        P(),
        P(),
        P(),
    )
    return jax.shard_map(
        shards, mesh=mesh, in_specs=in_specs, out_specs=P(("seq", "tp"), None), check_vma=False
    )
```

```python
import math

import jax
import jax.numpy as jnp
from jax import lax
from jax.experimental import pallas as pl
from jax.experimental.pallas import tpu as pltpu
from jax.sharding import PartitionSpec as P

MESH = pl.DeviceIdType.MESH
D = 4608
HD = 128
CTX = 1024
QR = 512
HALO = 4
CH = 64
NCH = CTX // CH
GR = 256
NP = 6
PC = D // NP
BF = jnp.bfloat16
F32 = jnp.float32
SCALE = 144 ** (-0.5)
EXP_SCALE = 50.0 * math.log2(math.e)
TO_Z, TO_X, TO_C1, TO_C3 = range(4)
SLOT = {TO_Z: 4, TO_X: 2, TO_C1: 1, TO_C3: 3}
PIECES = (0, 3, 1, 4, 2, 5)


def layer(
    gain_in, post_in, starts_in, counts_in, hid_in, wq_in, k_in, v_in, wo_in, out,
    gain, post, starts, counts, hid, nrm, wq, kbuf, vbuf, qbuf, acc, att, attr, wo, wp, part, rs_s, rs_r, obuf,
    hid_sem, load_sem, kv_s, kv_r, w_s, w_r, att_s, att_r, rss_sem, rsr_sem,
):
    s = lax.axis_index("seq")
    t = lax.axis_index("tp")
    c = s % 2
    xl = (s // 2) % 2
    z = s // 4
    xh = t % 2
    y = t // 2

    def dev(z_=None, xl_=None, c_=None, y_=None, xh_=None):
        z_ = z if z_ is None else z_
        xl_ = xl if xl_ is None else xl_
        c_ = c if c_ is None else c_
        y_ = y if y_ is None else y_
        xh_ = xh if xh_ is None else xh_
        return (z_ * 4 + xl_ * 2 + c_, y_ * 2 + xh_)

    z_up = dev(z_=(z + 1) % 4)
    z_down = dev(z_=(z + 3) % 4)
    x_near = dev(xl_=1 - xl)
    core = dev(c_=1 - c)
    x_far = dev(xh_=1 - xh)
    cross = dev(xl_=1 - xl, xh_=1 - xh)
    y_up = dev(y_=(y + 1) % 4)
    y_down = dev(y_=(y + 3) % 4)

    def block_row(slot_delta):
        return ((y + slot_delta) % 4) * 128

    loads = []
    for slot, delta in enumerate((3, 1, 2, 0)):
        rows = pl.ds(pl.multiple_of(block_row(delta), 128), 128)
        loads.append(
            pltpu.make_async_copy(hid_in.at[rows, :], hid.at[pl.ds(slot * 128, 128), :], hid_sem.at[slot])
        )
    load_wq = pltpu.make_async_copy(wq_in, wq, load_sem.at[0])
    load_k = pltpu.make_async_copy(k_in, kbuf.at[0], load_sem.at[1])
    load_v = pltpu.make_async_copy(v_in, vbuf.at[0], load_sem.at[2])
    load_wo = pltpu.make_async_copy(wo_in, wo, load_sem.at[3])
    load_gain = pltpu.make_async_copy(gain_in, gain, load_sem.at[4])
    small = [
        pltpu.make_async_copy(post_in, post, load_sem.at[5]),
        pltpu.make_async_copy(starts_in, starts, load_sem.at[6]),
        pltpu.make_async_copy(counts_in, counts, load_sem.at[7]),
    ]
    load_gain.start()
    for load in loads:
        load.start()
    load_wq.start()
    for load in small:
        load.start()

    barrier = pltpu.get_barrier_semaphore()
    for other in (z_up, z_down, x_near, core, x_far, cross, y_up, y_down):
        pl.semaphore_signal(barrier, inc=1, device_id=other, device_id_type=MESH)
    pl.semaphore_wait(barrier, 8)

    def remote(src, dst, send, recv, to):
        return pltpu.make_async_remote_copy(
            src_ref=src, dst_ref=dst, send_sem=send, recv_sem=recv, device_id=to, device_id_type=MESH
        )

    kv_to = {TO_Z: z_up, TO_X: x_near, TO_C1: core, TO_C3: core}

    GROUPED = (TO_C1, TO_C3)
    FIRST_SEM = {TO_Z: 0, TO_X: NCH, TO_C1: 2 * NCH, TO_C3: 2 * NCH + NCH // 4}

    def kv_send(stream, j, src):
        slot = SLOT[stream]
        rows = pl.ds(j * CH, CH)
        arrived = kv_r.at[FIRST_SEM[stream] + (j // 4 if stream in GROUPED else j)]
        for whole, buf in ((k_in, kbuf), (v_in, vbuf)):
            source = whole.at[rows, :] if src is None else buf.at[src, rows, :]
            remote(source, buf.at[slot, rows, :], kv_s.at[stream], arrived, kv_to[stream]).start()

    def kv_wait(stream, j):
        ref = kbuf.at[SLOT[stream], pl.ds(0, 8 * CH if stream in GROUPED else 2 * CH), :]
        remote(ref, ref, kv_s.at[stream], kv_r.at[FIRST_SEM[stream] + j], kv_to[stream]).wait_recv()

    def kv_sent(stream):
        ref = kbuf.at[pl.ds(0, 2)]
        remote(ref, ref, kv_s.at[stream], kv_r.at[FIRST_SEM[stream]], kv_to[stream]).wait_send()

    parity = z % 2
    W_CROSS, W_DOWN, W_CA, W_CB = range(4)
    w_to = {W_CROSS: cross, W_DOWN: z_down, W_CA: core, W_CB: core}

    def w_copy(stream, j, quarter, from_input=False):
        rows = pl.ds(pl.multiple_of(quarter * 128, 128), 128)
        cols = pl.ds(PIECES[j] * PC, PC)
        src = wo_in.at[rows, cols] if from_input else wp.at[rows, cols]
        return remote(src, wp.at[rows, cols], w_s.at[stream], w_r.at[stream, j], w_to[stream])

    def w_sent(stream):
        ref = wp.at[pl.ds(0, 128), :]
        remote(ref, ref, w_s.at[stream], w_r.at[stream, 0], w_to[stream]).wait_send()

    mine = parity * 2 + c
    above = (1 - parity) * 2 + c
    w_arrives = {
        W_CROSS: mine,
        W_DOWN: above,
        W_CA: parity * 2 + (1 - c),
        W_CB: (1 - parity) * 2 + (1 - c),
    }

    for j in range(NCH):
        kv_send(TO_Z, j, None)

        @pl.when(xl == 0)
        def _():
            kv_send(TO_X, j, None)

        @pl.when(c == 0)
        def _():
            kv_send(TO_C1, j, None)

        if j < NP:
            w_copy(W_CROSS, j, mine, from_input=True).start()
    load_k.start()
    load_v.start()
    load_wo.start()

    def step_f(j):
        kv_wait(TO_Z, j)

        @pl.when(xl == 1)
        def _():
            kv_send(TO_X, j, 4)

        @pl.when(c == 1)
        def _():
            kv_send(TO_C3, j, 4)

    def step_g(j):
        kv_wait(TO_X, j)

        @pl.when(c == 0)
        def _():
            kv_send(TO_C3, j, 2)

        @pl.when(c == 1)
        def _():
            kv_send(TO_C1, j, 2)

    def step_e(j):
        if j % 4 == 3:
            kv_wait(TO_C1, j // 4)
            kv_wait(TO_C3, j // 4)

    def step_w(j):
        w_copy(W_CROSS, j, mine).wait_recv()
        w_copy(W_DOWN, j, mine).start()
        w_copy(W_CA, j, mine).start()

    def step_z(j):
        w_copy(W_DOWN, j, above).wait_recv()
        w_copy(W_CB, j, above).start()

    def norm_rows(i, carry):
        rows = pl.ds(pl.multiple_of(i * 16, 16), 16)
        x = hid[rows, :].astype(F32)
        r = lax.rsqrt(jnp.mean(x * x, axis=-1, keepdims=True) + 0.1)
        nrm[rows, :] = (x * r * gain[...].reshape(1, D)).astype(BF)
        return carry

    done = dict.fromkeys((step_f, step_g, step_e, step_w, step_z), 0)

    def upto(step, n):
        for j in range(done[step], n):
            step(j)
        done[step] = max(done[step], n)

    load_gain.wait()
    for slot in range(4):
        loads[slot].wait()
        lax.fori_loop(slot * 8, slot * 8 + 8, norm_rows, 0, unroll=4)
    load_wq.wait()
    for m in range(2):
        q = jnp.dot(nrm[m * 256 : m * 256 + 256, :], wq[...], preferred_element_type=F32)
        q = (q * SCALE).astype(BF)
        for u in range(2):
            slot = 2 * m + u
            for kh in range(2):
                for g in range(2):
                    head = 2 * kh + g
                    qbuf[kh, slot * 256 + g * 128 : slot * 256 + g * 128 + 128, :] = q[
                        u * 128 : u * 128 + 128, head * HD : head * HD + HD
                    ]
    acc[...] = jnp.zeros_like(acc)
    for load in small:
        load.wait()
    load_k.wait()
    load_v.wait()

    off = starts[s] - s * CTX
    filled = {}
    for d in range(1, HALO + 1):
        source = s - d
        filled[d] = jnp.where(source >= 0, counts[jnp.maximum(source, 0)], 0)

    def attend(base, kh, tile, sources=(1, 2, 3, 0)):
        lanes = slice(kh * HD, kh * HD + HD)
        rows = slice(tile * 512, tile * 512 + 512)
        q = qbuf[kh, rows, :]
        row_ids = lax.broadcasted_iota(jnp.int32, (GR, HD), 0)

        def scores(d):
            key = kbuf[d, base : base + GR, lanes]
            return lax.dot_general(q, key, (((1,), (1,)), ((), ())), preferred_element_type=F32)

        def weights(x):
            return jnp.exp2(jnp.tanh(x * (1.0 / 50.0)) * EXP_SCALE)

        def values(d):
            v = vbuf[d, base : base + GR, lanes]
            if d == 0:
                return jnp.concatenate([v, jnp.ones_like(v)], axis=1)
            keep_row = jnp.where(row_ids < filled[d] - base, 1.0, 0.0).astype(BF)
            return jnp.concatenate([v * keep_row, keep_row], axis=1)

        pattern = lax.broadcasted_iota(jnp.int32, (128, GR), 1) - lax.broadcasted_iota(jnp.int32, (128, GR), 0)
        total = None
        for d in sources:
            if d == 0:
                near, far = scores(0), scores(4)
                w_near, w_far = [], []
                for u in range(4):
                    limit = off + block_row((3, 1, 2, 0)[2 * tile + u // 2]) - base
                    is_near = pattern <= limit
                    part_rows = slice(u * 128, u * 128 + 128)
                    w = weights(jnp.where(is_near, near[part_rows], far[part_rows]))
                    w_near.append(jnp.where(is_near, w, 0.0).astype(BF))
                    w_far.append(jnp.where(is_near, 0.0, w).astype(BF))
                term = jnp.dot(jnp.concatenate(w_near, axis=0), values(0), preferred_element_type=F32)
                term = term + jnp.dot(jnp.concatenate(w_far, axis=0), values(4), preferred_element_type=F32)
            else:
                term = jnp.dot(weights(scores(d)).astype(BF), values(d), preferred_element_type=F32)
            total = term if total is None else total + term
        acc[kh, rows, :] += total

    def units(base, tile, sources=(1, 2, 3, 0)):
        for kh in range(2):
            attend(base, kh, tile, sources)

    upto(step_f, 2)
    upto(step_w, 1)
    upto(step_f, 4)
    upto(step_g, 1)
    upto(step_f, 5)
    upto(step_g, 2)
    upto(step_f, 6)
    upto(step_w, 2)
    upto(step_g, 4)
    upto(step_f, 7)
    upto(step_e, 4)
    units(0, 0)
    upto(step_f, 9)
    upto(step_g, 5)
    upto(step_z, 1)
    units(0, 1)
    upto(step_w, 3)
    upto(step_f, 10)
    upto(step_g, 7)
    upto(step_f, 11)
    upto(step_g, 8)
    upto(step_z, 2)
    upto(step_e, 8)
    units(256, 0)
    upto(step_f, 13)
    upto(step_w, 4)
    upto(step_g, 10)
    units(256, 1)
    upto(step_f, 14)
    upto(step_g, 11)
    upto(step_z, 3)
    upto(step_f, 15)
    upto(step_g, 12)
    upto(step_w, 5)
    upto(step_e, 12)
    units(512, 0)
    upto(step_f, 16)
    upto(step_g, 14)
    units(512, 1)
    upto(step_w, 6)
    upto(step_z, 4)
    upto(step_g, 15)
    units(768, 0, (0,))
    upto(step_g, 16)
    units(768, 1, (0, 2))
    upto(step_e, 16)

    def att_copy(slot, kh):
        rows = pl.ds(pl.multiple_of((1 - xh) * 64, 64), 64)
        cols = pl.ds(kh * 256, 256)
        return remote(
            att.at[slot, rows, cols], attr.at[slot, :, cols], att_s, att_r.at[slot, kh], x_far
        )

    def finish(kh, tile):
        a = acc[kh, tile * 512 : tile * 512 + 512, :]
        o = (a[:, :HD] / a[:, HD:]).astype(BF)
        for u in range(4):
            head = kh * 2 + u % 2
            att[2 * tile + u // 2, :, head * HD : head * HD + HD] = o[u * 128 : u * 128 + 128, :]
        for slot in (2 * tile, 2 * tile + 1):
            att_copy(slot, kh).start()

    attend(768, 0, 0, (1, 2, 3))
    finish(0, 0)
    attend(768, 1, 0, (1, 2, 3))
    finish(1, 0)
    upto(step_z, 5)
    units(768, 1, (1, 3))
    finish(0, 1)
    finish(1, 1)

    def rs_copy(step, p):
        to = y_up if p < NP // 2 else y_down
        return remote(rs_s.at[step, p], rs_r.at[step, p], rss_sem.at[0 if p < NP // 2 else 1], rsr_sem.at[step, p], to)

    own_rows = pl.ds(pl.multiple_of(xh * 64, 64), 64)
    load_wo.wait()
    lhs = jnp.concatenate([att[slot, own_rows, :] for slot in range(4)], axis=0)
    for p in PIECES:
        cols = slice(p * PC, p * PC + PC)
        r = jnp.dot(lhs, wo[:, cols], preferred_element_type=F32)
        for slot in range(4):
            part[slot, :, cols] = r[slot * 64 : slot * 64 + 64]
    for tile in range(2):
        for slot in (2 * tile, 2 * tile + 1):
            for kh in range(2):
                att_copy(slot, kh).wait_recv()
        lhs_far = jnp.concatenate([attr[2 * tile], attr[2 * tile + 1]], axis=0)
        for j, p in enumerate(PIECES):
            if tile == 0:
                upto(step_z, j + 1)
                w_copy(W_CA, j, w_arrives[W_CA]).wait_recv()
                w_copy(W_CB, j, w_arrives[W_CB]).wait_recv()
            cols = slice(p * PC, p * PC + PC)
            r = jnp.dot(lhs_far, wp[:, cols], preferred_element_type=F32)
            if tile == 0:
                first, later = (0, 1) if p < NP // 2 else (1, 0)
                rs_s[0, p] = (part[first, :, cols] + r[first * 64 : first * 64 + 64]).astype(BF)
                rs_copy(0, p).start()
                part[later, :, cols] += r[later * 64 : later * 64 + 64]
            else:
                part[2, :, cols] += r[:64]
                part[3, :, cols] += r[64:]

    for step in (1, 2):
        for p in PIECES:
            cols = slice(p * PC, p * PC + PC)
            mine_slot = 2 if step == 1 else (1 if p < NP // 2 else 0)
            rs_copy(step - 1, p).wait_recv()
            rs_s[step, p] = (rs_r[step - 1, p].astype(F32) + part[mine_slot, :, cols]).astype(BF)
            rs_copy(step, p).start()
    squares = jnp.zeros((64, 1), F32)
    for p in PIECES:
        cols = slice(p * PC, p * PC + PC)
        rs_copy(2, p).wait_recv()
        whole = rs_r[2, p].astype(F32) + part[3, :, cols]
        part[3, :, cols] = whole
        squares = squares + jnp.sum(whole * whole, axis=-1, keepdims=True)
    factor = lax.rsqrt(squares * (1.0 / D) + 0.1)
    residual_rows = pl.ds(pl.multiple_of(384 + xh * 64, 64), 64)
    stores = []
    for p in range(NP):
        cols = slice(p * PC, p * PC + PC)
        residual = hid[residual_rows, cols].astype(F32)
        obuf[:, cols] = (residual + part[3, :, cols] * factor * post[cols].reshape(1, PC)).astype(BF)
    stores.append(pltpu.make_async_copy(obuf, out, load_sem.at[0]))
    for store in stores:
        store.start()
    for stream in (TO_Z, TO_X, TO_C1, TO_C3):
        kv_sent(stream)
    for stream in (W_CROSS, W_DOWN, W_CA, W_CB):
        w_sent(stream)
    remote(attr, attr, att_s, att_r.at[0, 0], x_far).wait_send()
    half = rs_s.at[:, pl.ds(0, NP // 2)]
    remote(half, half, rss_sem.at[0], rsr_sem.at[0, 0], y_up).wait_send()
    remote(half, half, rss_sem.at[1], rsr_sem.at[0, 0], y_down).wait_send()
    for store in stores:
        store.wait()


def shards(hidden_in, pre_gain, w_query, key_cache, value_cache, w_out, post_gain, starts, counts):
    hbm = pl.BlockSpec(memory_space=pltpu.HBM)
    dma = pltpu.SemaphoreType.DMA
    return pl.pallas_call(
        layer,
        out_shape=jax.ShapeDtypeStruct((64, D), BF),
        in_specs=[hbm] * 9,
        out_specs=hbm,
        scratch_shapes=[
            pltpu.VMEM((D,), F32),
            pltpu.VMEM((D,), F32),
            pltpu.SMEM((16,), jnp.int32),
            pltpu.SMEM((16,), jnp.int32),
            pltpu.VMEM((QR, D), BF),
            pltpu.VMEM((QR, D), BF),
            pltpu.VMEM((D, 512), BF),
            pltpu.VMEM((HALO + 1, CTX, 256), BF),
            pltpu.VMEM((HALO + 1, CTX, 256), BF),
            pltpu.VMEM((2, 1024, HD), BF),
            pltpu.VMEM((2, 1024, 256), F32),
            pltpu.VMEM((4, 128, 512), BF),
            pltpu.VMEM((4, 64, 512), BF),
            pltpu.VMEM((512, D), BF),
            pltpu.VMEM((512, D), BF),
            pltpu.VMEM((4, 64, D), F32),
            pltpu.VMEM((3, NP, 64, PC), BF),
            pltpu.VMEM((3, NP, 64, PC), BF),
            pltpu.VMEM((64, D), BF),
            dma((4,)),
            dma((8,)),
            dma((4,)),
            dma((2 * NCH + NCH // 2,)),
            dma((4,)),
            dma((4, NP)),
            dma,
            dma((4, 2)),
            dma((2,)),
            dma((3, NP)),
        ],
        compiler_params=pltpu.CompilerParams(
            collective_id=0, has_side_effects=True, vmem_limit_bytes=60 * 1024 * 1024
        ),
        name="layer",
    )(
        pre_gain, post_gain, starts, counts,
        hidden_in, w_query, key_cache, value_cache, w_out,
    )


def solution(mesh):
    in_specs = (
        P("seq", None),
        P(),
        P(None, "tp"),
        P("seq", "tp"),
        P("seq", "tp"),
        P("tp", None),
        P(),
        P(),
        P(),
    )
    return jax.shard_map(
        shards, mesh=mesh, in_specs=in_specs, out_specs=P(("seq", "tp"), None), check_vma=False
    )
```

```python
import math

import jax
import jax.numpy as jnp
from jax import lax
from jax.experimental import pallas as pl
from jax.experimental.pallas import tpu as pltpu
from jax.sharding import PartitionSpec as P

MESH = pl.DeviceIdType.MESH
D = 4608
HD = 128
CTX = 1024
QR = 512
HALO = 4
CHUNKS = tuple((64 * i, 64) for i in range(15)) + ((960, 32), (992, 32))
NCH = len(CHUNKS)
GROUPS = ((0, 4), (4, 8), (8, 12), (12, 14), (14, NCH))
GR = 256
NP = 6
PC = D // NP
BF = jnp.bfloat16
F32 = jnp.float32
SCALE = 144 ** (-0.5)
EXP_SCALE = 50.0 * math.log2(math.e)
TO_Z, TO_X, TO_C1, TO_C3 = range(4)
SLOT = {TO_Z: 4, TO_X: 2, TO_C1: 1, TO_C3: 3}
PIECES = (0, 3, 1, 4, 2, 5)


def layer(
    gain_in, post_in, starts_in, counts_in, hid_in, wq_in, k_in, v_in, wo_in, out,
    gain, post, starts, counts, hid, nrm, wq, kbuf, vbuf, qbuf, acc, att, attr, wo, wp, part, rs_s, rs_r,
    hid_sem, load_sem, kv_s, kv_r, w_s, w_r, att_s, att_r, rss_sem, rsr_sem,
):
    s = lax.axis_index("seq")
    t = lax.axis_index("tp")
    c = s % 2
    xl = (s // 2) % 2
    z = s // 4
    xh = t % 2
    y = t // 2

    def dev(z_=None, xl_=None, c_=None, y_=None, xh_=None):
        z_ = z if z_ is None else z_
        xl_ = xl if xl_ is None else xl_
        c_ = c if c_ is None else c_
        y_ = y if y_ is None else y_
        xh_ = xh if xh_ is None else xh_
        return (z_ * 4 + xl_ * 2 + c_, y_ * 2 + xh_)

    z_up = dev(z_=(z + 1) % 4)
    z_down = dev(z_=(z + 3) % 4)
    x_near = dev(xl_=1 - xl)
    core = dev(c_=1 - c)
    x_far = dev(xh_=1 - xh)
    cross = dev(xl_=1 - xl, xh_=1 - xh)
    y_up = dev(y_=(y + 1) % 4)
    y_down = dev(y_=(y + 3) % 4)

    def block_row(slot_delta):
        return ((y + slot_delta) % 4) * 128

    loads = []
    for slot, delta in enumerate((3, 1, 2, 0)):
        rows = pl.ds(pl.multiple_of(block_row(delta), 128), 128)
        loads.append(
            pltpu.make_async_copy(hid_in.at[rows, :], hid.at[pl.ds(slot * 128, 128), :], hid_sem.at[slot])
        )
    load_wq = pltpu.make_async_copy(wq_in, wq, load_sem.at[0])
    load_k = pltpu.make_async_copy(k_in, kbuf.at[0], load_sem.at[1])
    load_v = pltpu.make_async_copy(v_in, vbuf.at[0], load_sem.at[2])
    load_wo = pltpu.make_async_copy(wo_in, wo, load_sem.at[3])
    load_gain = pltpu.make_async_copy(gain_in, gain, load_sem.at[4])
    small = [
        pltpu.make_async_copy(post_in, post, load_sem.at[5]),
        pltpu.make_async_copy(starts_in, starts, load_sem.at[6]),
        pltpu.make_async_copy(counts_in, counts, load_sem.at[7]),
    ]
    load_gain.start()
    for load in loads:
        load.start()
    load_wq.start()
    for load in small:
        load.start()

    barrier = pltpu.get_barrier_semaphore()
    for other in (z_up, z_down, x_near, core, x_far, cross, y_up, y_down):
        pl.semaphore_signal(barrier, inc=1, device_id=other, device_id_type=MESH)
    pl.semaphore_wait(barrier, 8)

    def remote(src, dst, send, recv, to):
        return pltpu.make_async_remote_copy(
            src_ref=src, dst_ref=dst, send_sem=send, recv_sem=recv, device_id=to, device_id_type=MESH
        )

    kv_to = {TO_Z: z_up, TO_X: x_near, TO_C1: core, TO_C3: core}

    GROUPED = (TO_C1, TO_C3)
    FIRST_SEM = {TO_Z: 0, TO_X: NCH, TO_C1: 2 * NCH, TO_C3: 2 * NCH + len(GROUPS)}

    def kv_send(stream, j, src):
        slot = SLOT[stream]
        rows = pl.ds(*CHUNKS[j])
        place = next(g for g, (_, stop) in enumerate(GROUPS) if j < stop) if stream in GROUPED else j
        arrived = kv_r.at[FIRST_SEM[stream] + place]
        for whole, buf in ((k_in, kbuf), (v_in, vbuf)):
            source = whole.at[rows, :] if src is None else buf.at[src, rows, :]
            remote(source, buf.at[slot, rows, :], kv_s.at[stream], arrived, kv_to[stream]).start()

    def kv_wait(stream, j):
        first, stop = GROUPS[j] if stream in GROUPED else (j, j + 1)
        ref = kbuf.at[SLOT[stream], pl.ds(0, 2 * sum(n for _, n in CHUNKS[first:stop])), :]
        remote(ref, ref, kv_s.at[stream], kv_r.at[FIRST_SEM[stream] + j], kv_to[stream]).wait_recv()

    def kv_sent(stream):
        ref = kbuf.at[pl.ds(0, 2)]
        remote(ref, ref, kv_s.at[stream], kv_r.at[FIRST_SEM[stream]], kv_to[stream]).wait_send()

    parity = z % 2
    W_CROSS, W_DOWN, W_CA, W_CB = range(4)
    w_to = {W_CROSS: cross, W_DOWN: z_down, W_CA: core, W_CB: core}

    def w_copy(stream, j, quarter, from_input=False):
        rows = pl.ds(pl.multiple_of(quarter * 128, 128), 128)
        cols = pl.ds(PIECES[j] * PC, PC)
        src = wo_in.at[rows, cols] if from_input else wp.at[rows, cols]
        return remote(src, wp.at[rows, cols], w_s.at[stream], w_r.at[stream, j], w_to[stream])

    def w_sent(stream):
        ref = wp.at[pl.ds(0, 128), :]
        remote(ref, ref, w_s.at[stream], w_r.at[stream, 0], w_to[stream]).wait_send()

    mine = parity * 2 + c
    above = (1 - parity) * 2 + c
    w_arrives = {
        W_CROSS: mine,
        W_DOWN: above,
        W_CA: parity * 2 + (1 - c),
        W_CB: (1 - parity) * 2 + (1 - c),
    }

    stand_in = [
        pltpu.make_async_copy(k_in, kbuf.at[4], load_sem.at[8]),
        pltpu.make_async_copy(v_in, vbuf.at[4], load_sem.at[9]),
    ]
    stand_in_x = [
        pltpu.make_async_copy(k_in, kbuf.at[2], load_sem.at[10]),
        pltpu.make_async_copy(v_in, vbuf.at[2], load_sem.at[11]),
    ]
    first = z == 0
    first_two = (z * 2 + xl) == 0

    @pl.when(first)
    def _():
        for load in stand_in:
            load.start()

    @pl.when(first_two)
    def _():
        for load in stand_in_x:
            load.start()

    for j in range(NCH):
        @pl.when(z < 3)
        def _():
            kv_send(TO_Z, j, None)

        @pl.when(xl == 0)
        def _():
            kv_send(TO_X, j, None)

        @pl.when(c == 0)
        def _():
            kv_send(TO_C1, j, None)

        if j < NP:
            w_copy(W_CROSS, j, mine, from_input=True).start()
    load_k.start()
    load_v.start()
    load_wo.start()

    def step_f(j):
        @pl.when(z > 0)
        def _():
            kv_wait(TO_Z, j)

        if j == 0:
            @pl.when(first)
            def _():
                for load in stand_in:
                    load.wait()

        @pl.when((xl == 1) & (z > 0))
        def _():
            kv_send(TO_X, j, 4)

        @pl.when(c == 1)
        def _():
            kv_send(TO_C3, j, 4)

    def step_g(j):
        @pl.when(z * 2 + xl > 0)
        def _():
            kv_wait(TO_X, j)

        if j == 0:
            @pl.when(first_two)
            def _():
                for load in stand_in_x:
                    load.wait()

        @pl.when(c == 0)
        def _():
            kv_send(TO_C3, j, 2)

        @pl.when(c == 1)
        def _():
            kv_send(TO_C1, j, 2)

    def step_e(j):
        kv_wait(TO_C1, j)
        kv_wait(TO_C3, j)

    def step_w(j):
        w_copy(W_CROSS, j, mine).wait_recv()
        w_copy(W_DOWN, j, mine).start()
        w_copy(W_CA, j, mine).start()

    def step_z(j):
        w_copy(W_DOWN, j, above).wait_recv()
        w_copy(W_CB, j, above).start()

    def norm_rows(i, carry):
        rows = pl.ds(pl.multiple_of(i * 16, 16), 16)
        x = hid[rows, :].astype(F32)
        r = lax.rsqrt(jnp.mean(x * x, axis=-1, keepdims=True) + 0.1)
        nrm[rows, :] = (x * r * gain[...].reshape(1, D)).astype(BF)
        return carry

    done = dict.fromkeys((step_f, step_g, step_e, step_w, step_z), 0)

    def upto(step, n):
        for j in range(done[step], n):
            step(j)
        done[step] = max(done[step], n)

    load_gain.wait()
    for slot in range(4):
        loads[slot].wait()
        lax.fori_loop(slot * 8, slot * 8 + 8, norm_rows, 0, unroll=4)
    load_wq.wait()
    for m in range(2):
        q = jnp.dot(nrm[m * 256 : m * 256 + 256, :], wq[...], preferred_element_type=F32)
        q = (q * SCALE).astype(BF)
        for u in range(2):
            slot = 2 * m + u
            for kh in range(2):
                for g in range(2):
                    head = 2 * kh + g
                    qbuf[kh, slot * 256 + g * 128 : slot * 256 + g * 128 + 128, :] = q[
                        u * 128 : u * 128 + 128, head * HD : head * HD + HD
                    ]
    acc[...] = jnp.zeros_like(acc)
    for load in small:
        load.wait()
    load_k.wait()
    load_v.wait()

    off = starts[s] - s * CTX
    filled = {}
    for d in range(1, HALO + 1):
        source = s - d
        filled[d] = jnp.where(source >= 0, counts[jnp.maximum(source, 0)], 0)

    def attend(kh, tile, terms):
        lanes = slice(kh * HD, kh * HD + HD)
        rows = slice(tile * 512, tile * 512 + 512)
        q = qbuf[kh, rows, :]

        def scores(term):
            key = [kbuf[d, base : base + n, lanes] for d, base, n in term]
            key = key[0] if len(key) == 1 else jnp.concatenate(key, axis=0)
            return lax.dot_general(q, key, (((1,), (1,)), ((), ())), preferred_element_type=F32)

        def weights(x):
            return jnp.exp2(jnp.tanh(x * (1.0 / 50.0)) * EXP_SCALE)

        def values(term):
            out_rows = []
            for d, base, n in term:
                v = vbuf[d, base : base + n, lanes]
                if d == 0:
                    out_rows.append(jnp.concatenate([v, jnp.ones_like(v)], axis=1))
                else:
                    row_ids = lax.broadcasted_iota(jnp.int32, (n, HD), 0)
                    keep_row = jnp.where(row_ids < filled[d] - base, 1.0, 0.0).astype(BF)
                    out_rows.append(jnp.concatenate([v * keep_row, keep_row], axis=1))
            return out_rows[0] if len(out_rows) == 1 else jnp.concatenate(out_rows, axis=0)

        total = None
        for term in terms:
            if term[0][0] == 0:
                _, base, n = term[0]
                pattern = lax.broadcasted_iota(jnp.int32, (128, n), 1) - lax.broadcasted_iota(jnp.int32, (128, n), 0)
                near, far = scores(((0, base, n),)), scores(((4, base, n),))
                w_near, w_far = [], []
                for u in range(4):
                    limit = off + block_row((3, 1, 2, 0)[2 * tile + u // 2]) - base
                    is_near = pattern <= limit
                    part_rows = slice(u * 128, u * 128 + 128)
                    w = weights(jnp.where(is_near, near[part_rows], far[part_rows]))
                    w_near.append(jnp.where(is_near, w, 0.0).astype(BF))
                    w_far.append(jnp.where(is_near, 0.0, w).astype(BF))
                add = jnp.dot(
                    jnp.concatenate(w_near, axis=0), values(((0, base, n),)), preferred_element_type=F32
                )
                add = add + jnp.dot(
                    jnp.concatenate(w_far, axis=0), values(((4, base, n),)), preferred_element_type=F32
                )
            else:
                add = jnp.dot(weights(scores(term)).astype(BF), values(term), preferred_element_type=F32)
            total = add if total is None else total + add
        acc[kh, rows, :] += total

    def single(base, *distances):
        return tuple(((d, base, GR),) for d in distances)

    def units(tile, terms):
        for kh in range(2):
            attend(kh, tile, terms)

    LAST_A = (((1, 768, 128), (3, 768, 128)),)
    LAST_B = (((1, 896, 128), (3, 896, 128)),)

    upto(step_f, 4)
    upto(step_w, 1)
    upto(step_g, 1)
    upto(step_f, 5)
    upto(step_g, 2)
    upto(step_f, 6)
    upto(step_g, 3)
    upto(step_w, 2)
    upto(step_f, 7)
    upto(step_g, 4)
    upto(step_e, 1)
    units(0, single(0, 1, 2, 3, 0))
    upto(step_f, 9)
    upto(step_g, 5)
    upto(step_z, 1)
    units(1, single(0, 1, 2, 3, 0))
    upto(step_f, 10)
    upto(step_g, 7)
    upto(step_w, 3)
    upto(step_f, 11)
    upto(step_g, 8)
    upto(step_z, 2)
    upto(step_e, 2)
    units(0, single(256, 1, 2, 3, 0))
    upto(step_f, 13)
    upto(step_g, 10)
    upto(step_w, 4)
    units(1, single(256, 1, 2, 3, 0))
    upto(step_f, 14)
    upto(step_g, 11)
    upto(step_f, 15)
    upto(step_g, 12)
    upto(step_w, 5)
    upto(step_z, 3)
    upto(step_e, 3)
    units(0, single(512, 1, 2, 3, 0))
    upto(step_f, NCH)
    upto(step_g, 14)
    units(0, single(768, 0))
    upto(step_g, 15)
    upto(step_w, 6)
    upto(step_e, 4)
    units(0, LAST_A)
    upto(step_g, NCH)
    upto(step_z, 4)
    units(0, single(768, 2))
    upto(step_e, 5)

    def att_copy(slot, kh):
        rows = pl.ds(pl.multiple_of((1 - xh) * 64, 64), 64)
        cols = pl.ds(kh * 256, 256)
        return remote(
            att.at[slot, rows, cols], attr.at[slot, :, cols], att_s, att_r.at[slot, kh], x_far
        )

    def finish(kh, tile):
        a = acc[kh, tile * 512 : tile * 512 + 512, :]
        o = (a[:, :HD] / a[:, HD:]).astype(BF)
        for u in range(4):
            head = kh * 2 + u % 2
            att[2 * tile + u // 2, :, head * HD : head * HD + HD] = o[u * 128 : u * 128 + 128, :]
        for slot in (2 * tile, 2 * tile + 1):
            att_copy(slot, kh).start()

    attend(0, 0, LAST_B)
    finish(0, 0)
    attend(1, 0, LAST_B)
    finish(1, 0)
    units(1, single(512, 1, 2, 3, 0))
    upto(step_z, 5)
    units(1, single(768, 1, 2, 3, 0))
    finish(0, 1)
    finish(1, 1)

    def rs_copy(step, p):
        to = y_up if p < NP // 2 else y_down
        return remote(rs_s.at[step, p], rs_r.at[step, p], rss_sem.at[0 if p < NP // 2 else 1], rsr_sem.at[step, p], to)

    own_rows = pl.ds(pl.multiple_of(xh * 64, 64), 64)
    load_wo.wait()

    def own_part(tile, p):
        lhs = jnp.concatenate([att[2 * tile, own_rows, :], att[2 * tile + 1, own_rows, :]], axis=0)
        return jnp.dot(lhs, wo[:, p * PC : p * PC + PC], preferred_element_type=F32)

    def far_part(tile, p):
        lhs = jnp.concatenate([attr[2 * tile], attr[2 * tile + 1]], axis=0)
        return jnp.dot(lhs, wp[:, p * PC : p * PC + PC], preferred_element_type=F32)

    def att_arrived(tile):
        for slot in (2 * tile, 2 * tile + 1):
            for kh in range(2):
                att_copy(slot, kh).wait_recv()

    for p in PIECES:
        cols = slice(p * PC, p * PC + PC)
        r = own_part(0, p)
        part[0, :, cols] = r[:64]
        part[1, :, cols] = r[64:]
    upto(step_z, 6)
    att_arrived(0)
    for j, p in enumerate(PIECES):
        w_copy(W_CA, j, w_arrives[W_CA]).wait_recv()
        w_copy(W_CB, j, w_arrives[W_CB]).wait_recv()
        cols = slice(p * PC, p * PC + PC)
        r = far_part(0, p)
        first, later = (0, 1) if p < NP // 2 else (1, 0)
        rs_s[0, p] = (part[first, :, cols] + r[first * 64 : first * 64 + 64]).astype(BF)
        rs_copy(0, p).start()
        part[later, :, cols] += r[later * 64 : later * 64 + 64]
    att_arrived(1)
    for step in (1, 2):
        for p in PIECES:
            cols = slice(p * PC, p * PC + PC)
            if step == 1:
                r = own_part(1, p) + far_part(1, p)
                part[2, :, cols] = r[:64]
                part[3, :, cols] = r[64:]
            mine_slot = 2 if step == 1 else (1 if p < NP // 2 else 0)
            rs_copy(step - 1, p).wait_recv()
            rs_s[step, p] = (rs_r[step - 1, p].astype(F32) + part[mine_slot, :, cols]).astype(BF)
            rs_copy(step, p).start()
    squares = jnp.zeros((64, 1), F32)
    for p in PIECES:
        cols = slice(p * PC, p * PC + PC)
        rs_copy(2, p).wait_recv()
        whole = rs_r[2, p].astype(F32) + part[3, :, cols]
        part[3, :, cols] = whole
        squares = squares + jnp.sum(whole * whole, axis=-1, keepdims=True)
    factor = lax.rsqrt(squares * (1.0 / D) + 0.1)
    residual_rows = pl.ds(pl.multiple_of(384 + xh * 64, 64), 64)
    for p in range(NP):
        cols = slice(p * PC, p * PC + PC)
        residual = hid[residual_rows, cols].astype(F32)
        out[:, cols] = (residual + part[3, :, cols] * factor * post[cols].reshape(1, PC)).astype(BF)
    @pl.when(z < 3)
    def _():
        kv_sent(TO_Z)

    @pl.when((xl == 0) | (z > 0))
    def _():
        kv_sent(TO_X)

    for stream in (TO_C1, TO_C3):
        kv_sent(stream)
    for stream in (W_CROSS, W_DOWN, W_CA, W_CB):
        w_sent(stream)
    remote(attr, attr, att_s, att_r.at[0, 0], x_far).wait_send()
    half = rs_s.at[:, pl.ds(0, NP // 2)]
    remote(half, half, rss_sem.at[0], rsr_sem.at[0, 0], y_up).wait_send()
    remote(half, half, rss_sem.at[1], rsr_sem.at[0, 0], y_down).wait_send()


def shards(hidden_in, pre_gain, w_query, key_cache, value_cache, w_out, post_gain, starts, counts):
    hbm = pl.BlockSpec(memory_space=pltpu.HBM)
    dma = pltpu.SemaphoreType.DMA
    return pl.pallas_call(
        layer,
        out_shape=jax.ShapeDtypeStruct((64, D), BF),
        in_specs=[hbm] * 9,
        out_specs=pl.BlockSpec(memory_space=pltpu.VMEM),
        scratch_shapes=[
            pltpu.VMEM((D,), F32),
            pltpu.VMEM((D,), F32),
            pltpu.SMEM((16,), jnp.int32),
            pltpu.SMEM((16,), jnp.int32),
            pltpu.VMEM((QR, D), BF),
            pltpu.VMEM((QR, D), BF),
            pltpu.VMEM((D, 512), BF),
            pltpu.VMEM((HALO + 1, CTX, 256), BF),
            pltpu.VMEM((HALO + 1, CTX, 256), BF),
            pltpu.VMEM((2, 1024, HD), BF),
            pltpu.VMEM((2, 1024, 256), F32),
            pltpu.VMEM((4, 128, 512), BF),
            pltpu.VMEM((4, 64, 512), BF),
            pltpu.VMEM((512, D), BF),
            pltpu.VMEM((512, D), BF),
            pltpu.VMEM((4, 64, D), F32),
            pltpu.VMEM((3, NP, 64, PC), BF),
            pltpu.VMEM((3, NP, 64, PC), BF),
            dma((4,)),
            dma((12,)),
            dma((4,)),
            dma((2 * NCH + 2 * len(GROUPS),)),
            dma((4,)),
            dma((4, NP)),
            dma,
            dma((4, 2)),
            dma((2,)),
            dma((3, NP)),
        ],
        compiler_params=pltpu.CompilerParams(
            collective_id=0, has_side_effects=True, vmem_limit_bytes=50 * 1024 * 1024
        ),
        name="layer",
    )(
        *[
            pltpu.with_memory_space_constraint(x, pltpu.HBM)
            for x in (
                pre_gain, post_gain, starts, counts,
                hidden_in, w_query, key_cache, value_cache, w_out,
            )
        ]
    )


def solution(mesh):
    in_specs = (
        P("seq", None),
        P(),
        P(None, "tp"),
        P("seq", "tp"),
        P("seq", "tp"),
        P("tp", None),
        P(),
        P(),
        P(),
    )
    return jax.shard_map(
        shards, mesh=mesh, in_specs=in_specs, out_specs=P(("seq", "tp"), None), check_vma=False
    )
```

```python
import math

import jax
import jax.numpy as jnp
from jax import lax
from jax.experimental import pallas as pl
from jax.experimental.pallas import tpu as pltpu
from jax.sharding import PartitionSpec as P

MESH = pl.DeviceIdType.MESH
D = 4608
HD = 128
CTX = 1024
QR = 512
HALO = 4
CHUNKS = ((0, 32), (32, 32)) + tuple((64 * i, 64) for i in range(1, 15)) + ((960, 32), (992, 32))
NCH = len(CHUNKS)
GROUPS = ((0, 5), (5, 9), (9, 13), (13, 15), (15, NCH))
GR = 256
NP = 6
PC = D // NP
BF = jnp.bfloat16
F32 = jnp.float32
SCALE = 144 ** (-0.5)
EXP_SCALE = 50.0 * math.log2(math.e)
TO_Z, TO_X, TO_C1, TO_C3 = range(4)
SLOT = {TO_Z: 4, TO_X: 2, TO_C1: 1, TO_C3: 3}
PIECES = (0, 3, 1, 4, 2, 5)


def layer(
    gain_in, post_in, starts_in, counts_in, hid_in, wq_in, k_in, v_in, wo_in, out,
    gain, post, starts, counts, hid, nrm, wq, kbuf, vbuf, qbuf, acc, att, attr, wo, wp, part, rs_s, rs_r,
    hid_sem, load_sem, kv_s, kv_r, w_s, w_r, att_s, att_r, rss_sem, rsr_sem,
):
    s = lax.axis_index("seq")
    t = lax.axis_index("tp")
    c = s % 2
    xl = (s // 2) % 2
    z = s // 4
    xh = t % 2
    y = t // 2

    def dev(z_=None, xl_=None, c_=None, y_=None, xh_=None):
        z_ = z if z_ is None else z_
        xl_ = xl if xl_ is None else xl_
        c_ = c if c_ is None else c_
        y_ = y if y_ is None else y_
        xh_ = xh if xh_ is None else xh_
        return (z_ * 4 + xl_ * 2 + c_, y_ * 2 + xh_)

    z_up = dev(z_=(z + 1) % 4)
    z_down = dev(z_=(z + 3) % 4)
    x_near = dev(xl_=1 - xl)
    core = dev(c_=1 - c)
    x_far = dev(xh_=1 - xh)
    cross = dev(xl_=1 - xl, xh_=1 - xh)
    y_up = dev(y_=(y + 1) % 4)
    y_down = dev(y_=(y + 3) % 4)

    def block_row(slot_delta):
        return ((y + slot_delta) % 4) * 128

    loads = []
    for slot, delta in enumerate((3, 1, 2, 0)):
        rows = pl.ds(pl.multiple_of(block_row(delta), 128), 128)
        loads.append(
            pltpu.make_async_copy(hid_in.at[rows, :], hid.at[pl.ds(slot * 128, 128), :], hid_sem.at[slot])
        )
    load_wq = pltpu.make_async_copy(wq_in, wq, load_sem.at[0])
    load_k = pltpu.make_async_copy(k_in, kbuf.at[0], load_sem.at[1])
    load_v = pltpu.make_async_copy(v_in, vbuf.at[0], load_sem.at[2])
    load_wo = pltpu.make_async_copy(wo_in, wo, load_sem.at[3])
    load_gain = pltpu.make_async_copy(gain_in, gain, load_sem.at[4])
    small = [
        pltpu.make_async_copy(post_in, post, load_sem.at[5]),
        pltpu.make_async_copy(starts_in, starts, load_sem.at[6]),
        pltpu.make_async_copy(counts_in, counts, load_sem.at[7]),
    ]
    load_gain.start()
    for load in loads:
        load.start()
    load_wq.start()
    for load in small:
        load.start()

    barrier = pltpu.get_barrier_semaphore()
    for other in (z_up, z_down, x_near, core, x_far, cross, y_up, y_down):
        pl.semaphore_signal(barrier, inc=1, device_id=other, device_id_type=MESH)
    pl.semaphore_wait(barrier, 8)

    def remote(src, dst, send, recv, to):
        return pltpu.make_async_remote_copy(
            src_ref=src, dst_ref=dst, send_sem=send, recv_sem=recv, device_id=to, device_id_type=MESH
        )

    kv_to = {TO_Z: z_up, TO_X: x_near, TO_C1: core, TO_C3: core}

    GROUPED = (TO_C1, TO_C3)
    FIRST_SEM = {TO_Z: 0, TO_X: NCH, TO_C1: 2 * NCH, TO_C3: 2 * NCH + len(GROUPS)}

    def kv_send(stream, j, src):
        slot = SLOT[stream]
        rows = pl.ds(*CHUNKS[j])
        place = next(g for g, (_, stop) in enumerate(GROUPS) if j < stop) if stream in GROUPED else j
        arrived = kv_r.at[FIRST_SEM[stream] + place]
        for whole, buf in ((k_in, kbuf), (v_in, vbuf)):
            source = whole.at[rows, :] if src is None else buf.at[src, rows, :]
            remote(source, buf.at[slot, rows, :], kv_s.at[stream], arrived, kv_to[stream]).start()

    def kv_wait(stream, j):
        first, stop = GROUPS[j] if stream in GROUPED else (j, j + 1)
        ref = kbuf.at[SLOT[stream], pl.ds(0, 2 * sum(n for _, n in CHUNKS[first:stop])), :]
        remote(ref, ref, kv_s.at[stream], kv_r.at[FIRST_SEM[stream] + j], kv_to[stream]).wait_recv()

    def kv_sent(stream):
        ref = kbuf.at[pl.ds(0, 2)]
        remote(ref, ref, kv_s.at[stream], kv_r.at[FIRST_SEM[stream]], kv_to[stream]).wait_send()

    parity = z % 2
    W_CROSS, W_DOWN, W_CA, W_CB = range(4)
    w_to = {W_CROSS: cross, W_DOWN: z_down, W_CA: core, W_CB: core}

    def w_copy(stream, j, quarter, from_input=False):
        rows = pl.ds(pl.multiple_of(quarter * 128, 128), 128)
        cols = pl.ds(PIECES[j] * PC, PC)
        src = wo_in.at[rows, cols] if from_input else wp.at[rows, cols]
        return remote(src, wp.at[rows, cols], w_s.at[stream], w_r.at[stream, j], w_to[stream])

    def w_sent(stream):
        ref = wp.at[pl.ds(0, 128), :]
        remote(ref, ref, w_s.at[stream], w_r.at[stream, 0], w_to[stream]).wait_send()

    mine = parity * 2 + c
    above = (1 - parity) * 2 + c
    w_arrives = {
        W_CROSS: mine,
        W_DOWN: above,
        W_CA: parity * 2 + (1 - c),
        W_CB: (1 - parity) * 2 + (1 - c),
    }

    stand_in = [
        pltpu.make_async_copy(k_in, kbuf.at[4], load_sem.at[8]),
        pltpu.make_async_copy(v_in, vbuf.at[4], load_sem.at[9]),
    ]
    stand_in_x = [
        pltpu.make_async_copy(k_in, kbuf.at[2], load_sem.at[10]),
        pltpu.make_async_copy(v_in, vbuf.at[2], load_sem.at[11]),
    ]
    first = z == 0
    first_two = (z * 2 + xl) == 0

    for j in range(NCH):
        @pl.when(z < 3)
        def _():
            kv_send(TO_Z, j, None)

        @pl.when(xl == 0)
        def _():
            kv_send(TO_X, j, None)

        @pl.when(c == 0)
        def _():
            kv_send(TO_C1, j, None)

        if j < NP:
            w_copy(W_CROSS, j, mine, from_input=True).start()

    @pl.when(first)
    def _():
        for load in stand_in:
            load.start()

    @pl.when(first_two)
    def _():
        for load in stand_in_x:
            load.start()

    load_k.start()
    load_v.start()
    load_wo.start()

    def step_f(j):
        @pl.when(z > 0)
        def _():
            kv_wait(TO_Z, j)

        if j == 0:
            @pl.when(first)
            def _():
                for load in stand_in:
                    load.wait()

        @pl.when((xl == 1) & (z > 0))
        def _():
            kv_send(TO_X, j, 4)

        @pl.when(c == 1)
        def _():
            kv_send(TO_C3, j, 4)

    def step_g(j):
        @pl.when(z * 2 + xl > 0)
        def _():
            kv_wait(TO_X, j)

        if j == 0:
            @pl.when(first_two)
            def _():
                for load in stand_in_x:
                    load.wait()

        @pl.when(c == 0)
        def _():
            kv_send(TO_C3, j, 2)

        @pl.when(c == 1)
        def _():
            kv_send(TO_C1, j, 2)

    def step_e(j):
        kv_wait(TO_C1, j)
        kv_wait(TO_C3, j)

    def step_w(j):
        w_copy(W_CROSS, j, mine).wait_recv()
        w_copy(W_DOWN, j, mine).start()
        w_copy(W_CA, j, mine).start()

    def step_z(j):
        w_copy(W_DOWN, j, above).wait_recv()
        w_copy(W_CB, j, above).start()

    def norm_rows(i, carry):
        rows = pl.ds(pl.multiple_of(i * 16, 16), 16)
        x = hid[rows, :].astype(F32)
        r = lax.rsqrt(jnp.mean(x * x, axis=-1, keepdims=True) + 0.1)
        nrm[rows, :] = (x * r * gain[...].reshape(1, D)).astype(BF)
        return carry

    done = dict.fromkeys((step_f, step_g, step_e, step_w, step_z), 0)

    def upto(step, n):
        for j in range(done[step], n):
            step(j)
        done[step] = max(done[step], n)

    load_gain.wait()
    for slot in range(4):
        loads[slot].wait()
        lax.fori_loop(slot * 8, slot * 8 + 8, norm_rows, 0, unroll=4)
    load_wq.wait()
    for slot in range(4):
        q = jnp.dot(nrm[slot * 128 : slot * 128 + 128, :], wq[...], preferred_element_type=F32)
        q = (q * SCALE).astype(BF)
        for kh in range(2):
            for g in range(2):
                head = 2 * kh + g
                qbuf[kh, slot * 256 + g * 128 : slot * 256 + g * 128 + 128, :] = q[
                    :, head * HD : head * HD + HD
                ]
        if slot == 1:
            upto(step_f, 1)
        if slot == 2:
            upto(step_f, 2)
    acc[...] = jnp.zeros_like(acc)
    for load in small:
        load.wait()
    load_k.wait()
    load_v.wait()

    off = starts[s] - s * CTX
    filled = {}
    for d in range(1, HALO + 1):
        source = s - d
        filled[d] = jnp.where(source >= 0, counts[jnp.maximum(source, 0)], 0)

    def attend(kh, tile, terms):
        lanes = slice(kh * HD, kh * HD + HD)
        rows = slice(tile * 512, tile * 512 + 512)
        q = qbuf[kh, rows, :]

        def scores(term):
            key = [kbuf[d, base : base + n, lanes] for d, base, n in term]
            key = key[0] if len(key) == 1 else jnp.concatenate(key, axis=0)
            return lax.dot_general(q, key, (((1,), (1,)), ((), ())), preferred_element_type=F32)

        def weights(x):
            return jnp.exp2(jnp.tanh(x * (1.0 / 50.0)) * EXP_SCALE)

        def values(term):
            out_rows = []
            for d, base, n in term:
                v = vbuf[d, base : base + n, lanes]
                if d == 0:
                    out_rows.append(jnp.concatenate([v, jnp.ones_like(v)], axis=1))
                else:
                    row_ids = lax.broadcasted_iota(jnp.int32, (n, HD), 0)
                    keep_row = jnp.where(row_ids < filled[d] - base, 1.0, 0.0).astype(BF)
                    out_rows.append(jnp.concatenate([v * keep_row, keep_row], axis=1))
            return out_rows[0] if len(out_rows) == 1 else jnp.concatenate(out_rows, axis=0)

        total = None
        for term in terms:
            if term[0][0] == 0:
                _, base, n = term[0]
                pattern = lax.broadcasted_iota(jnp.int32, (128, n), 1) - lax.broadcasted_iota(jnp.int32, (128, n), 0)
                near, far = scores(((0, base, n),)), scores(((4, base, n),))
                w_near, w_far = [], []
                for u in range(4):
                    limit = off + block_row((3, 1, 2, 0)[2 * tile + u // 2]) - base
                    is_near = pattern <= limit
                    part_rows = slice(u * 128, u * 128 + 128)
                    w = weights(jnp.where(is_near, near[part_rows], far[part_rows]))
                    w_near.append(jnp.where(is_near, w, 0.0).astype(BF))
                    w_far.append(jnp.where(is_near, 0.0, w).astype(BF))
                add = jnp.dot(
                    jnp.concatenate(w_near, axis=0), values(((0, base, n),)), preferred_element_type=F32
                )
                add = add + jnp.dot(
                    jnp.concatenate(w_far, axis=0), values(((4, base, n),)), preferred_element_type=F32
                )
            else:
                add = jnp.dot(weights(scores(term)).astype(BF), values(term), preferred_element_type=F32)
            total = add if total is None else total + add
        acc[kh, rows, :] += total

    def single(base, *distances):
        return tuple(((d, base, GR),) for d in distances)

    def units(tile, terms):
        for kh in range(2):
            attend(kh, tile, terms)

    LAST_A = (((1, 768, 128), (3, 768, 128)),)
    LAST_B = (((1, 896, 128), (3, 896, 128)),)

    upto(step_f, 5)
    upto(step_w, 1)
    upto(step_g, 2)
    upto(step_f, 6)
    upto(step_g, 3)
    upto(step_f, 7)
    upto(step_g, 4)
    upto(step_f, 8)
    upto(step_g, 5)
    upto(step_w, 2)
    upto(step_e, 1)
    units(0, single(0, 1, 2, 3, 0))
    upto(step_f, 10)
    upto(step_g, 6)
    units(1, single(0, 1, 2, 3, 0))
    upto(step_f, 11)
    upto(step_g, 8)
    upto(step_w, 3)
    upto(step_f, 12)
    upto(step_g, 9)
    upto(step_z, 1)
    upto(step_e, 2)
    units(0, single(256, 1, 2, 3, 0))
    upto(step_f, 14)
    upto(step_g, 11)
    upto(step_w, 4)
    units(1, single(256, 1, 2, 3, 0))
    upto(step_f, 15)
    upto(step_g, 12)
    upto(step_z, 2)
    upto(step_f, 16)
    upto(step_g, 13)
    upto(step_w, 5)
    upto(step_e, 3)
    units(0, single(512, 1, 2, 3, 0))
    upto(step_f, NCH)
    upto(step_g, 15)
    upto(step_z, 3)
    units(0, single(768, 0))
    upto(step_g, 16)
    upto(step_e, 4)
    units(0, LAST_A)
    upto(step_g, NCH)
    upto(step_w, 6)
    units(0, single(768, 2))
    upto(step_e, 5)

    def att_copy(slot, kh):
        rows = pl.ds(pl.multiple_of((1 - xh) * 64, 64), 64)
        cols = pl.ds(kh * 256, 256)
        return remote(
            att.at[slot, rows, cols], attr.at[slot, :, cols], att_s, att_r.at[slot, kh], x_far
        )

    def finish(kh, tile):
        a = acc[kh, tile * 512 : tile * 512 + 512, :]
        o = (a[:, :HD] / a[:, HD:]).astype(BF)
        for u in range(4):
            head = kh * 2 + u % 2
            att[2 * tile + u // 2, :, head * HD : head * HD + HD] = o[u * 128 : u * 128 + 128, :]
        for slot in (2 * tile, 2 * tile + 1):
            att_copy(slot, kh).start()

    attend(0, 0, LAST_B)
    finish(0, 0)
    attend(1, 0, LAST_B)
    finish(1, 0)
    upto(step_z, 4)
    units(1, single(512, 1, 2, 3, 0))
    units(1, single(768, 1, 2, 3, 0))
    upto(step_z, 5)
    finish(0, 1)
    finish(1, 1)

    def rs_copy(step, p):
        to = y_up if p < NP // 2 else y_down
        return remote(rs_s.at[step, p], rs_r.at[step, p], rss_sem.at[0 if p < NP // 2 else 1], rsr_sem.at[step, p], to)

    own_rows = pl.ds(pl.multiple_of(xh * 64, 64), 64)
    load_wo.wait()

    def own_part(tile, p):
        lhs = jnp.concatenate([att[2 * tile, own_rows, :], att[2 * tile + 1, own_rows, :]], axis=0)
        return jnp.dot(lhs, wo[:, p * PC : p * PC + PC], preferred_element_type=F32)

    def far_part(tile, p):
        lhs = jnp.concatenate([attr[2 * tile], attr[2 * tile + 1]], axis=0)
        return jnp.dot(lhs, wp[:, p * PC : p * PC + PC], preferred_element_type=F32)

    def att_arrived(tile):
        for slot in (2 * tile, 2 * tile + 1):
            for kh in range(2):
                att_copy(slot, kh).wait_recv()

    for p in PIECES:
        cols = slice(p * PC, p * PC + PC)
        r = own_part(0, p)
        part[0, :, cols] = r[:64]
        part[1, :, cols] = r[64:]
    att_arrived(0)
    for j, p in enumerate(PIECES):
        if j == 4:
            upto(step_z, 6)
        w_copy(W_CA, j, w_arrives[W_CA]).wait_recv()
        w_copy(W_CB, j, w_arrives[W_CB]).wait_recv()
        cols = slice(p * PC, p * PC + PC)
        r = far_part(0, p)
        first, later = (0, 1) if p < NP // 2 else (1, 0)
        rs_s[0, p] = (part[first, :, cols] + r[first * 64 : first * 64 + 64]).astype(BF)
        rs_copy(0, p).start()
        part[later, :, cols] += r[later * 64 : later * 64 + 64]
    att_arrived(1)
    for step in (1, 2):
        for p in PIECES:
            cols = slice(p * PC, p * PC + PC)
            if step == 1:
                r = own_part(1, p) + far_part(1, p)
                part[2, :, cols] = r[:64]
                part[3, :, cols] = r[64:]
            mine_slot = 2 if step == 1 else (1 if p < NP // 2 else 0)
            rs_copy(step - 1, p).wait_recv()
            rs_s[step, p] = (rs_r[step - 1, p].astype(F32) + part[mine_slot, :, cols]).astype(BF)
            rs_copy(step, p).start()
    squares = jnp.zeros((64, 1), F32)
    for p in PIECES:
        cols = slice(p * PC, p * PC + PC)
        rs_copy(2, p).wait_recv()
        whole = rs_r[2, p].astype(F32) + part[3, :, cols]
        part[3, :, cols] = whole
        squares = squares + jnp.sum(whole * whole, axis=-1, keepdims=True)
    factor = lax.rsqrt(squares * (1.0 / D) + 0.1)
    residual_rows = pl.ds(pl.multiple_of(384 + xh * 64, 64), 64)
    for p in range(NP):
        cols = slice(p * PC, p * PC + PC)
        residual = hid[residual_rows, cols].astype(F32)
        out[:, cols] = (residual + part[3, :, cols] * factor * post[cols].reshape(1, PC)).astype(BF)
    @pl.when(z < 3)
    def _():
        kv_sent(TO_Z)

    @pl.when((xl == 0) | (z > 0))
    def _():
        kv_sent(TO_X)

    for stream in (TO_C1, TO_C3):
        kv_sent(stream)
    for stream in (W_CROSS, W_DOWN, W_CA, W_CB):
        w_sent(stream)
    remote(attr, attr, att_s, att_r.at[0, 0], x_far).wait_send()
    half = rs_s.at[:, pl.ds(0, NP // 2)]
    remote(half, half, rss_sem.at[0], rsr_sem.at[0, 0], y_up).wait_send()
    remote(half, half, rss_sem.at[1], rsr_sem.at[0, 0], y_down).wait_send()


def shards(hidden_in, pre_gain, w_query, key_cache, value_cache, w_out, post_gain, starts, counts):
    hbm = pl.BlockSpec(memory_space=pltpu.HBM)
    dma = pltpu.SemaphoreType.DMA
    return pl.pallas_call(
        layer,
        out_shape=jax.ShapeDtypeStruct((64, D), BF),
        in_specs=[hbm] * 9,
        out_specs=pl.BlockSpec(memory_space=pltpu.VMEM),
        scratch_shapes=[
            pltpu.VMEM((D,), F32),
            pltpu.VMEM((D,), F32),
            pltpu.SMEM((16,), jnp.int32),
            pltpu.SMEM((16,), jnp.int32),
            pltpu.VMEM((QR, D), BF),
            pltpu.VMEM((QR, D), BF),
            pltpu.VMEM((D, 512), BF),
            pltpu.VMEM((HALO + 1, CTX, 256), BF),
            pltpu.VMEM((HALO + 1, CTX, 256), BF),
            pltpu.VMEM((2, 1024, HD), BF),
            pltpu.VMEM((2, 1024, 256), F32),
            pltpu.VMEM((4, 128, 512), BF),
            pltpu.VMEM((4, 64, 512), BF),
            pltpu.VMEM((512, D), BF),
            pltpu.VMEM((512, D), BF),
            pltpu.VMEM((4, 64, D), F32),
            pltpu.VMEM((3, NP, 64, PC), BF),
            pltpu.VMEM((3, NP, 64, PC), BF),
            dma((4,)),
            dma((12,)),
            dma((4,)),
            dma((2 * NCH + 2 * len(GROUPS),)),
            dma((4,)),
            dma((4, NP)),
            dma,
            dma((4, 2)),
            dma((2,)),
            dma((3, NP)),
        ],
        compiler_params=pltpu.CompilerParams(
            collective_id=0, has_side_effects=True, vmem_limit_bytes=50 * 1024 * 1024
        ),
        name="layer",
    )(
        *[
            pltpu.with_memory_space_constraint(x, pltpu.HBM)
            for x in (
                pre_gain, post_gain, starts, counts,
                hidden_in, w_query, key_cache, value_cache, w_out,
            )
        ]
    )


def solution(mesh):
    in_specs = (
        P("seq", None),
        P(),
        P(None, "tp"),
        P("seq", "tp"),
        P("seq", "tp"),
        P("tp", None),
        P(),
        P(),
        P(),
    )
    return jax.shard_map(
        shards, mesh=mesh, in_specs=in_specs, out_specs=P(("seq", "tp"), None), check_vma=False
    )
```

```python
import math

import jax
import jax.numpy as jnp
from jax import lax
from jax.experimental import pallas as pl
from jax.experimental.pallas import tpu as pltpu
from jax.sharding import PartitionSpec as P

MESH = pl.DeviceIdType.MESH
D = 4608
HD = 128
CTX = 1024
QR = 512
HALO = 4
CHUNKS = ((0, 32), (32, 32)) + tuple((64 * i, 64) for i in range(1, 15)) + ((960, 32), (992, 32))
NCH = len(CHUNKS)
DIRECT = (16, 17)
DIRECT_ROWS = sum(CHUNKS[j][1] for j in DIRECT)
GROUPS = ((0, 5), (5, 9), (9, 13), (13, 15), (15, NCH))
GR = 256
NP = 6
PC = D // NP
BF = jnp.bfloat16
F32 = jnp.float32
SCALE = 144 ** (-0.5)
EXP_SCALE = 50.0 * math.log2(math.e)
TO_Z, TO_X, TO_C1, TO_C3 = range(4)
SLOT = {TO_Z: 4, TO_X: 2, TO_C1: 1, TO_C3: 3}
PIECES = (0, 3, 1, 4, 2, 5)


def layer(
    gain_in, post_in, starts_in, counts_in, hid_in, wq_in, k_in, v_in, wo_in, out,
    gain, post, starts, counts, hid, nrm, wq, kbuf, vbuf, qbuf, acc, att, attr, wo, wp, part, rs_s, rs_r,
    hid_sem, load_sem, kv_s, kv_r, w_s, w_r, att_s, att_r, rss_sem, rsr_sem,
):
    s = lax.axis_index("seq")
    t = lax.axis_index("tp")
    c = s % 2
    xl = (s // 2) % 2
    z = s // 4
    xh = t % 2
    y = t // 2

    def dev(z_=None, xl_=None, c_=None, y_=None, xh_=None):
        z_ = z if z_ is None else z_
        xl_ = xl if xl_ is None else xl_
        c_ = c if c_ is None else c_
        y_ = y if y_ is None else y_
        xh_ = xh if xh_ is None else xh_
        return (z_ * 4 + xl_ * 2 + c_, y_ * 2 + xh_)

    z_up = dev(z_=(z + 1) % 4)
    z_down = dev(z_=(z + 3) % 4)
    x_near = dev(xl_=1 - xl)
    core = dev(c_=1 - c)
    x_far = dev(xh_=1 - xh)
    cross = dev(xl_=1 - xl, xh_=1 - xh)
    diagonal = dev(z_=(z + 3 - 2 * xl) % 4, xl_=1 - xl)
    y_up = dev(y_=(y + 1) % 4)
    y_down = dev(y_=(y + 3) % 4)

    def block_row(slot_delta):
        return ((y + slot_delta) % 4) * 128

    loads = []
    for slot, delta in enumerate((3, 1, 2, 0)):
        rows = pl.ds(pl.multiple_of(block_row(delta), 128), 128)
        loads.append(
            pltpu.make_async_copy(hid_in.at[rows, :], hid.at[pl.ds(slot * 128, 128), :], hid_sem.at[slot])
        )
    load_wq = pltpu.make_async_copy(wq_in, wq, load_sem.at[0])
    load_k = pltpu.make_async_copy(k_in, kbuf.at[0], load_sem.at[1])
    load_v = pltpu.make_async_copy(v_in, vbuf.at[0], load_sem.at[2])
    load_wo = pltpu.make_async_copy(wo_in, wo, load_sem.at[3])
    load_gain = pltpu.make_async_copy(gain_in, gain, load_sem.at[4])
    small = [
        pltpu.make_async_copy(post_in, post, load_sem.at[5]),
        pltpu.make_async_copy(starts_in, starts, load_sem.at[6]),
        pltpu.make_async_copy(counts_in, counts, load_sem.at[7]),
    ]
    load_gain.start()
    for load in loads:
        load.start()
    load_wq.start()
    for load in small:
        load.start()

    barrier = pltpu.get_barrier_semaphore()
    for other in (z_up, z_down, x_near, core, x_far, cross, diagonal, y_up, y_down):
        pl.semaphore_signal(barrier, inc=1, device_id=other, device_id_type=MESH)
    pl.semaphore_wait(barrier, 9)

    def remote(src, dst, send, recv, to):
        return pltpu.make_async_remote_copy(
            src_ref=src, dst_ref=dst, send_sem=send, recv_sem=recv, device_id=to, device_id_type=MESH
        )

    kv_to = {TO_Z: z_up, TO_X: x_near, TO_C1: core, TO_C3: core}

    GROUPED = (TO_C1, TO_C3)
    FIRST_SEM = {TO_Z: 0, TO_X: NCH, TO_C1: 2 * NCH, TO_C3: 2 * NCH + len(GROUPS)}

    def kv_send(stream, j, src):
        slot = SLOT[stream]
        rows = pl.ds(*CHUNKS[j])
        place = next(g for g, (_, stop) in enumerate(GROUPS) if j < stop) if stream in GROUPED else j
        arrived = kv_r.at[FIRST_SEM[stream] + place]
        for whole, buf in ((k_in, kbuf), (v_in, vbuf)):
            source = whole.at[rows, :] if src is None else buf.at[src, rows, :]
            remote(source, buf.at[slot, rows, :], kv_s.at[stream], arrived, kv_to[stream]).start()

    def kv_wait(stream, j):
        first, stop = GROUPS[j] if stream in GROUPED else (j, j + 1)
        ref = kbuf.at[SLOT[stream], pl.ds(0, 2 * sum(n for _, n in CHUNKS[first:stop])), :]
        remote(ref, ref, kv_s.at[stream], kv_r.at[FIRST_SEM[stream] + j], kv_to[stream]).wait_recv()

    def direct_send(j):
        rows = pl.ds(*CHUNKS[j])
        arrived = kv_r.at[FIRST_SEM[TO_X] + j]
        for whole, buf in ((k_in, kbuf), (v_in, vbuf)):
            remote(whole.at[rows, :], buf.at[SLOT[TO_X], rows, :], kv_s.at[4], arrived, diagonal).start()

    def kv_sent(stream, rows=CTX):
        ref = kbuf.at[pl.ds(0, 2), pl.ds(0, rows), :]
        to, first_sem = (diagonal, 0) if stream == 4 else (kv_to[stream], FIRST_SEM[stream])
        remote(ref, ref, kv_s.at[stream], kv_r.at[first_sem], to).wait_send()

    parity = z % 2
    W_CROSS, W_DOWN, W_CA, W_CB = range(4)
    w_to = {W_CROSS: cross, W_DOWN: z_down, W_CA: core, W_CB: core}

    def w_copy(stream, j, quarter, from_input=False):
        rows = pl.ds(pl.multiple_of(quarter * 128, 128), 128)
        cols = pl.ds(PIECES[j] * PC, PC)
        src = wo_in.at[rows, cols] if from_input else wp.at[rows, cols]
        return remote(src, wp.at[rows, cols], w_s.at[stream], w_r.at[stream, j], w_to[stream])

    def w_sent(stream):
        ref = wp.at[pl.ds(0, 128), :]
        remote(ref, ref, w_s.at[stream], w_r.at[stream, 0], w_to[stream]).wait_send()

    mine = parity * 2 + c
    above = (1 - parity) * 2 + c
    w_arrives = {
        W_CROSS: mine,
        W_DOWN: above,
        W_CA: parity * 2 + (1 - c),
        W_CB: (1 - parity) * 2 + (1 - c),
    }

    stand_in = [
        pltpu.make_async_copy(k_in, kbuf.at[4], load_sem.at[8]),
        pltpu.make_async_copy(v_in, vbuf.at[4], load_sem.at[9]),
    ]
    stand_in_x = [
        pltpu.make_async_copy(k_in, kbuf.at[2], load_sem.at[10]),
        pltpu.make_async_copy(v_in, vbuf.at[2], load_sem.at[11]),
    ]
    first = z == 0
    first_two = (z * 2 + xl) == 0

    @pl.when((xl == 1) & (z < 3))
    def _():
        for j in DIRECT:
            direct_send(j)

    for j in range(NCH):
        @pl.when(z < 3)
        def _():
            kv_send(TO_Z, j, None)

        @pl.when(xl == 0)
        def _():
            kv_send(TO_X, j, None)

        @pl.when(c == 0)
        def _():
            kv_send(TO_C1, j, None)

        if j < NP:
            w_copy(W_CROSS, j, mine, from_input=True).start()

    load_k.start()
    load_v.start()

    def step_f(j):
        @pl.when(z > 0)
        def _():
            kv_wait(TO_Z, j)

        if j == 0:
            @pl.when(first)
            def _():
                for load in stand_in:
                    load.wait()

        if j not in DIRECT:
            @pl.when((xl == 1) & (z > 0))
            def _():
                kv_send(TO_X, j, 4)

        @pl.when(c == 1)
        def _():
            kv_send(TO_C3, j, 4)

    def step_g(j):
        @pl.when(z * 2 + xl > 0)
        def _():
            kv_wait(TO_X, j)

        if j == 0:
            @pl.when(first_two)
            def _():
                for load in stand_in_x:
                    load.wait()

        @pl.when(c == 0)
        def _():
            kv_send(TO_C3, j, 2)

        @pl.when(c == 1)
        def _():
            kv_send(TO_C1, j, 2)

    def step_e(j):
        kv_wait(TO_C1, j)
        kv_wait(TO_C3, j)

    def step_w(j):
        w_copy(W_CROSS, j, mine).wait_recv()
        w_copy(W_DOWN, j, mine).start()
        w_copy(W_CA, j, mine).start()

    def step_z(j):
        w_copy(W_DOWN, j, above).wait_recv()
        w_copy(W_CB, j, above).start()

    def norm_rows(i, carry):
        rows = pl.ds(pl.multiple_of(i * 16, 16), 16)
        x = hid[rows, :].astype(F32)
        r = lax.rsqrt(jnp.mean(x * x, axis=-1, keepdims=True) + 0.1)
        nrm[rows, :] = (x * r * gain[...].reshape(1, D)).astype(BF)
        return carry

    done = dict.fromkeys((step_f, step_g, step_e, step_w, step_z), 0)

    def upto(step, n):
        for j in range(done[step], n):
            step(j)
        done[step] = max(done[step], n)

    load_gain.wait()
    for slot in range(4):
        loads[slot].wait()
        lax.fori_loop(slot * 8, slot * 8 + 8, norm_rows, 0, unroll=4)
    @pl.when(first)
    def _():
        for load in stand_in:
            load.start()

    @pl.when(first_two)
    def _():
        for load in stand_in_x:
            load.start()

    load_wo.start()
    load_wq.wait()
    for slot in range(4):
        q = jnp.dot(nrm[slot * 128 : slot * 128 + 128, :], wq[...], preferred_element_type=F32)
        q = (q * SCALE).astype(BF)
        for kh in range(2):
            for g in range(2):
                head = 2 * kh + g
                qbuf[kh, slot * 256 + g * 128 : slot * 256 + g * 128 + 128, :] = q[
                    :, head * HD : head * HD + HD
                ]
        if slot == 1:
            upto(step_f, 1)
        if slot == 2:
            upto(step_f, 2)
    acc[...] = jnp.zeros_like(acc)
    for load in small:
        load.wait()
    load_k.wait()
    load_v.wait()

    off = starts[s] - s * CTX
    filled = {}
    for d in range(1, HALO + 1):
        source = s - d
        filled[d] = jnp.where(source >= 0, counts[jnp.maximum(source, 0)], 0)

    def attend(kh, tile, terms):
        lanes = slice(kh * HD, kh * HD + HD)
        rows = slice(tile * 512, tile * 512 + 512)
        q = qbuf[kh, rows, :]

        def scores(term):
            key = [kbuf[d, base : base + n, lanes] for d, base, n in term]
            key = key[0] if len(key) == 1 else jnp.concatenate(key, axis=0)
            return lax.dot_general(q, key, (((1,), (1,)), ((), ())), preferred_element_type=F32)

        def weights(x):
            return jnp.exp2(jnp.tanh(x * (1.0 / 50.0)) * EXP_SCALE)

        def values(term):
            out_rows = []
            for d, base, n in term:
                v = vbuf[d, base : base + n, lanes]
                if d == 0:
                    out_rows.append(jnp.concatenate([v, jnp.ones_like(v)], axis=1))
                else:
                    row_ids = lax.broadcasted_iota(jnp.int32, (n, HD), 0)
                    keep_row = jnp.where(row_ids < filled[d] - base, 1.0, 0.0).astype(BF)
                    out_rows.append(jnp.concatenate([v * keep_row, keep_row], axis=1))
            return out_rows[0] if len(out_rows) == 1 else jnp.concatenate(out_rows, axis=0)

        total = None
        for term in terms:
            if term[0][0] == 0:
                _, base, n = term[0]
                pattern = lax.broadcasted_iota(jnp.int32, (128, n), 1) - lax.broadcasted_iota(jnp.int32, (128, n), 0)
                near, far = scores(((0, base, n),)), scores(((4, base, n),))
                w_near, w_far = [], []
                for u in range(4):
                    limit = off + block_row((3, 1, 2, 0)[2 * tile + u // 2]) - base
                    is_near = pattern <= limit
                    part_rows = slice(u * 128, u * 128 + 128)
                    w = weights(jnp.where(is_near, near[part_rows], far[part_rows]))
                    w_near.append(jnp.where(is_near, w, 0.0).astype(BF))
                    w_far.append(jnp.where(is_near, 0.0, w).astype(BF))
                add = jnp.dot(
                    jnp.concatenate(w_near, axis=0), values(((0, base, n),)), preferred_element_type=F32
                )
                add = add + jnp.dot(
                    jnp.concatenate(w_far, axis=0), values(((4, base, n),)), preferred_element_type=F32
                )
            else:
                add = jnp.dot(weights(scores(term)).astype(BF), values(term), preferred_element_type=F32)
            total = add if total is None else total + add
        acc[kh, rows, :] += total

    def single(base, *distances):
        return tuple(((d, base, GR),) for d in distances)

    def units(tile, terms):
        for kh in range(2):
            attend(kh, tile, terms)

    LAST_A = (((1, 768, 128), (3, 768, 128)),)
    LAST_B = (((1, 896, 128), (3, 896, 128)),)

    upto(step_f, 5)
    upto(step_w, 1)
    upto(step_g, 2)
    upto(step_f, 6)
    upto(step_g, 3)
    upto(step_f, 7)
    upto(step_g, 4)
    upto(step_f, 8)
    upto(step_g, 5)
    upto(step_w, 2)
    upto(step_e, 1)
    units(0, single(0, 1, 2, 3, 0))
    upto(step_f, 10)
    upto(step_g, 6)
    units(1, single(0, 1, 2, 3, 0))
    upto(step_f, 11)
    upto(step_g, 8)
    upto(step_w, 3)
    upto(step_f, 12)
    upto(step_g, 9)
    upto(step_z, 1)
    upto(step_e, 2)
    units(0, single(256, 1, 2, 3, 0))
    upto(step_f, 14)
    upto(step_g, 11)
    upto(step_w, 4)
    units(1, single(256, 1, 2, 3, 0))
    upto(step_f, 15)
    upto(step_g, 12)
    upto(step_z, 2)
    upto(step_f, 16)
    upto(step_g, 13)
    upto(step_w, 5)
    upto(step_e, 3)
    units(0, single(512, 1, 2, 3, 0))
    upto(step_f, NCH)
    upto(step_g, 15)
    upto(step_z, 3)
    units(0, single(768, 0))
    upto(step_g, 16)
    upto(step_e, 4)
    units(0, LAST_A)
    upto(step_g, NCH)
    upto(step_w, 6)
    units(0, single(768, 2))
    upto(step_e, 5)

    def att_copy(slot, kh):
        rows = pl.ds(pl.multiple_of((1 - xh) * 64, 64), 64)
        cols = pl.ds(kh * 256, 256)
        return remote(
            att.at[slot, rows, cols], attr.at[slot, :, cols], att_s, att_r.at[slot, kh], x_far
        )

    def finish(kh, tile):
        a = acc[kh, tile * 512 : tile * 512 + 512, :]
        o = (a[:, :HD] / a[:, HD:]).astype(BF)
        for u in range(4):
            head = kh * 2 + u % 2
            att[2 * tile + u // 2, :, head * HD : head * HD + HD] = o[u * 128 : u * 128 + 128, :]
        for slot in (2 * tile, 2 * tile + 1):
            att_copy(slot, kh).start()

    attend(0, 0, LAST_B)
    finish(0, 0)
    attend(1, 0, LAST_B)
    finish(1, 0)
    upto(step_z, 4)
    units(1, single(512, 1, 2, 3, 0))
    units(1, single(768, 1, 2, 3, 0))
    upto(step_z, 5)
    finish(0, 1)
    finish(1, 1)

    def rs_copy(step, p):
        to = y_up if p < NP // 2 else y_down
        return remote(rs_s.at[step, p], rs_r.at[step, p], rss_sem.at[0 if p < NP // 2 else 1], rsr_sem.at[step, p], to)

    own_rows = pl.ds(pl.multiple_of(xh * 64, 64), 64)
    load_wo.wait()

    def own_part(tile, p):
        lhs = jnp.concatenate([att[2 * tile, own_rows, :], att[2 * tile + 1, own_rows, :]], axis=0)
        return jnp.dot(lhs, wo[:, p * PC : p * PC + PC], preferred_element_type=F32)

    def far_part(tile, p):
        lhs = jnp.concatenate([attr[2 * tile], attr[2 * tile + 1]], axis=0)
        return jnp.dot(lhs, wp[:, p * PC : p * PC + PC], preferred_element_type=F32)

    def att_arrived(tile):
        for slot in (2 * tile, 2 * tile + 1):
            for kh in range(2):
                att_copy(slot, kh).wait_recv()

    for p in PIECES:
        cols = slice(p * PC, p * PC + PC)
        r = own_part(0, p)
        part[0, :, cols] = r[:64]
        part[1, :, cols] = r[64:]
    att_arrived(0)
    for j, p in enumerate(PIECES):
        if j == 4:
            upto(step_z, 6)
        w_copy(W_CA, j, w_arrives[W_CA]).wait_recv()
        w_copy(W_CB, j, w_arrives[W_CB]).wait_recv()
        cols = slice(p * PC, p * PC + PC)
        r = far_part(0, p)
        first, later = (0, 1) if p < NP // 2 else (1, 0)
        rs_s[0, p] = (part[first, :, cols] + r[first * 64 : first * 64 + 64]).astype(BF)
        rs_copy(0, p).start()
        part[later, :, cols] += r[later * 64 : later * 64 + 64]
    att_arrived(1)
    for step in (1, 2):
        for p in PIECES:
            cols = slice(p * PC, p * PC + PC)
            if step == 1:
                r = own_part(1, p) + far_part(1, p)
                part[2, :, cols] = r[:64]
                part[3, :, cols] = r[64:]
            mine_slot = 2 if step == 1 else (1 if p < NP // 2 else 0)
            rs_copy(step - 1, p).wait_recv()
            rs_s[step, p] = (rs_r[step - 1, p].astype(F32) + part[mine_slot, :, cols]).astype(BF)
            rs_copy(step, p).start()
    squares = jnp.zeros((64, 1), F32)
    for p in PIECES:
        cols = slice(p * PC, p * PC + PC)
        rs_copy(2, p).wait_recv()
        whole = rs_r[2, p].astype(F32) + part[3, :, cols]
        part[3, :, cols] = whole
        squares = squares + jnp.sum(whole * whole, axis=-1, keepdims=True)
    factor = lax.rsqrt(squares * (1.0 / D) + 0.1)
    residual_rows = pl.ds(pl.multiple_of(384 + xh * 64, 64), 64)
    for p in range(NP):
        cols = slice(p * PC, p * PC + PC)
        residual = hid[residual_rows, cols].astype(F32)
        out[:, cols] = (residual + part[3, :, cols] * factor * post[cols].reshape(1, PC)).astype(BF)
    @pl.when(z < 3)
    def _():
        kv_sent(TO_Z)

    @pl.when(xl == 0)
    def _():
        kv_sent(TO_X)

    @pl.when((xl == 1) & (z > 0))
    def _():
        kv_sent(TO_X, CTX - DIRECT_ROWS)

    @pl.when((xl == 1) & (z < 3))
    def _():
        kv_sent(4, DIRECT_ROWS)

    for stream in (TO_C1, TO_C3):
        kv_sent(stream)
    for stream in (W_CROSS, W_DOWN, W_CA, W_CB):
        w_sent(stream)
    remote(attr, attr, att_s, att_r.at[0, 0], x_far).wait_send()
    half = rs_s.at[:, pl.ds(0, NP // 2)]
    remote(half, half, rss_sem.at[0], rsr_sem.at[0, 0], y_up).wait_send()
    remote(half, half, rss_sem.at[1], rsr_sem.at[0, 0], y_down).wait_send()


def shards(hidden_in, pre_gain, w_query, key_cache, value_cache, w_out, post_gain, starts, counts):
    hbm = pl.BlockSpec(memory_space=pltpu.HBM)
    dma = pltpu.SemaphoreType.DMA
    return pl.pallas_call(
        layer,
        out_shape=jax.ShapeDtypeStruct((64, D), BF),
        in_specs=[hbm] * 9,
        out_specs=pl.BlockSpec(memory_space=pltpu.VMEM),
        scratch_shapes=[
            pltpu.VMEM((D,), F32),
            pltpu.VMEM((D,), F32),
            pltpu.SMEM((16,), jnp.int32),
            pltpu.SMEM((16,), jnp.int32),
            pltpu.VMEM((QR, D), BF),
            pltpu.VMEM((QR, D), BF),
            pltpu.VMEM((D, 512), BF),
            pltpu.VMEM((HALO + 1, CTX, 256), BF),
            pltpu.VMEM((HALO + 1, CTX, 256), BF),
            pltpu.VMEM((2, 1024, HD), BF),
            pltpu.VMEM((2, 1024, 256), F32),
            pltpu.VMEM((4, 128, 512), BF),
            pltpu.VMEM((4, 64, 512), BF),
            pltpu.VMEM((512, D), BF),
            pltpu.VMEM((512, D), BF),
            pltpu.VMEM((4, 64, D), F32),
            pltpu.VMEM((3, NP, 64, PC), BF),
            pltpu.VMEM((3, NP, 64, PC), BF),
            dma((4,)),
            dma((12,)),
            dma((5,)),
            dma((2 * NCH + 2 * len(GROUPS),)),
            dma((4,)),
            dma((4, NP)),
            dma,
            dma((4, 2)),
            dma((2,)),
            dma((3, NP)),
        ],
        compiler_params=pltpu.CompilerParams(
            collective_id=0, has_side_effects=True, vmem_limit_bytes=50 * 1024 * 1024
        ),
        name="layer",
    )(
        *[
            pltpu.with_memory_space_constraint(x, pltpu.HBM)
            for x in (
                pre_gain, post_gain, starts, counts,
                hidden_in, w_query, key_cache, value_cache, w_out,
            )
        ]
    )


def solution(mesh):
    in_specs = (
        P("seq", None),
        P(),
        P(None, "tp"),
        P("seq", "tp"),
        P("seq", "tp"),
        P("tp", None),
        P(),
        P(),
        P(),
    )
    return jax.shard_map(
        shards, mesh=mesh, in_specs=in_specs, out_specs=P(("seq", "tp"), None), check_vma=False
    )
```

```python
import math

import jax
import jax.numpy as jnp
from jax import lax
from jax.experimental import pallas as pl
from jax.experimental.pallas import tpu as pltpu
from jax.sharding import PartitionSpec as P

MESH = pl.DeviceIdType.MESH
D = 4608
HD = 128
CTX = 1024
QR = 512
HALO = 4
CHUNKS = ((0, 32), (32, 32)) + tuple((64 * i, 64) for i in range(1, 15)) + ((960, 32), (992, 32))
NCH = len(CHUNKS)
DIRECT = (16, 17)
DIRECT_ROWS = sum(CHUNKS[j][1] for j in DIRECT)
GROUPS = ((0, 5), (5, 9), (9, 13), (13, 15), (15, NCH))
GR = 256
NP = 6
PC = D // NP
BF = jnp.bfloat16
F32 = jnp.float32
SCALE = 144 ** (-0.5)
EXP_SCALE = 50.0 * math.log2(math.e)
TO_Z, TO_X, TO_C1, TO_C3 = range(4)
SLOT = {TO_Z: 4, TO_X: 2, TO_C1: 1, TO_C3: 3}
PIECES = (0, 3, 1, 4, 2, 5)


def layer(
    gain_in, post_in, starts_in, counts_in, hid_in, wq_in, k_in, v_in, wo_in, out,
    gain, post, starts, counts, hid, nrm, wq, kbuf, vbuf, qbuf, acc, att, attr, wo, wp, part, rs_s, rs_r,
    hid_sem, load_sem, kv_s, kv_r, w_s, w_r, att_s, att_r, rss_sem, rsr_sem,
):
    s = lax.axis_index("seq")
    t = lax.axis_index("tp")
    c = s % 2
    xl = (s // 2) % 2
    z = s // 4
    xh = t % 2
    y = t // 2

    def dev(z_=None, xl_=None, c_=None, y_=None, xh_=None):
        z_ = z if z_ is None else z_
        xl_ = xl if xl_ is None else xl_
        c_ = c if c_ is None else c_
        y_ = y if y_ is None else y_
        xh_ = xh if xh_ is None else xh_
        return (z_ * 4 + xl_ * 2 + c_, y_ * 2 + xh_)

    z_up = dev(z_=(z + 1) % 4)
    z_down = dev(z_=(z + 3) % 4)
    x_near = dev(xl_=1 - xl)
    core = dev(c_=1 - c)
    x_far = dev(xh_=1 - xh)
    cross = dev(xl_=1 - xl, xh_=1 - xh)
    diagonal = dev(z_=(z + 3 - 2 * xl) % 4, xl_=1 - xl)
    y_up = dev(y_=(y + 1) % 4)
    y_down = dev(y_=(y + 3) % 4)

    def block_row(slot_delta):
        return ((y + slot_delta) % 4) * 128

    loads = []
    for slot, delta in enumerate((3, 1, 2, 0)):
        rows = pl.ds(pl.multiple_of(block_row(delta), 128), 128)
        loads.append(
            pltpu.make_async_copy(hid_in.at[rows, :], hid.at[pl.ds(slot * 128, 128), :], hid_sem.at[slot])
        )
    load_wq = pltpu.make_async_copy(wq_in, wq, load_sem.at[0])
    load_k = pltpu.make_async_copy(k_in, kbuf.at[0], load_sem.at[1])
    load_v = pltpu.make_async_copy(v_in, vbuf.at[0], load_sem.at[2])
    load_wo = pltpu.make_async_copy(wo_in, wo, load_sem.at[3])
    load_gain = pltpu.make_async_copy(gain_in, gain, load_sem.at[4])
    small = [
        pltpu.make_async_copy(post_in, post, load_sem.at[5]),
        pltpu.make_async_copy(starts_in, starts, load_sem.at[6]),
        pltpu.make_async_copy(counts_in, counts, load_sem.at[7]),
    ]
    load_gain.start()
    for load in loads:
        load.start()
    load_wq.start()
    for load in small:
        load.start()

    barrier = pltpu.get_barrier_semaphore()
    for other in (z_up, z_down, x_near, core, x_far, cross, diagonal, y_up, y_down):
        pl.semaphore_signal(barrier, inc=1, device_id=other, device_id_type=MESH)
    pl.semaphore_wait(barrier, 9)

    def remote(src, dst, send, recv, to):
        return pltpu.make_async_remote_copy(
            src_ref=src, dst_ref=dst, send_sem=send, recv_sem=recv, device_id=to, device_id_type=MESH
        )

    kv_to = {TO_Z: z_up, TO_X: x_near, TO_C1: core, TO_C3: core}

    GROUPED = (TO_C1, TO_C3)
    FIRST_SEM = {TO_Z: 0, TO_X: NCH, TO_C1: 2 * NCH, TO_C3: 2 * NCH + len(GROUPS)}

    def kv_send(stream, j, src):
        slot = SLOT[stream]
        rows = pl.ds(*CHUNKS[j])
        place = next(g for g, (_, stop) in enumerate(GROUPS) if j < stop) if stream in GROUPED else j
        arrived = kv_r.at[FIRST_SEM[stream] + place]
        for whole, buf in ((k_in, kbuf), (v_in, vbuf)):
            source = whole.at[rows, :] if src is None else buf.at[src, rows, :]
            remote(source, buf.at[slot, rows, :], kv_s.at[stream], arrived, kv_to[stream]).start()

    def kv_wait(stream, j):
        first, stop = GROUPS[j] if stream in GROUPED else (j, j + 1)
        ref = kbuf.at[SLOT[stream], pl.ds(0, 2 * sum(n for _, n in CHUNKS[first:stop])), :]
        remote(ref, ref, kv_s.at[stream], kv_r.at[FIRST_SEM[stream] + j], kv_to[stream]).wait_recv()

    def direct_send(j):
        rows = pl.ds(*CHUNKS[j])
        arrived = kv_r.at[FIRST_SEM[TO_X] + j]
        for whole, buf in ((k_in, kbuf), (v_in, vbuf)):
            remote(whole.at[rows, :], buf.at[SLOT[TO_X], rows, :], kv_s.at[4], arrived, diagonal).start()

    def kv_sent(stream, rows=CTX):
        ref = kbuf.at[pl.ds(0, 2), pl.ds(0, rows), :]
        to, first_sem = (diagonal, 0) if stream == 4 else (kv_to[stream], FIRST_SEM[stream])
        remote(ref, ref, kv_s.at[stream], kv_r.at[first_sem], to).wait_send()

    parity = z % 2
    W_CROSS, W_DOWN, W_CA, W_CB = range(4)
    w_to = {W_CROSS: cross, W_DOWN: z_down, W_CA: core, W_CB: core}

    def w_copy(stream, j, quarter, from_input=False):
        rows = pl.ds(pl.multiple_of(quarter * 128, 128), 128)
        cols = pl.ds(PIECES[j] * PC, PC)
        src = wo_in.at[rows, cols] if from_input else wp.at[rows, cols]
        return remote(src, wp.at[rows, cols], w_s.at[stream], w_r.at[stream, j], w_to[stream])

    def w_sent(stream):
        ref = wp.at[pl.ds(0, 128), :]
        remote(ref, ref, w_s.at[stream], w_r.at[stream, 0], w_to[stream]).wait_send()

    mine = parity * 2 + c
    above = (1 - parity) * 2 + c
    w_arrives = {
        W_CROSS: mine,
        W_DOWN: above,
        W_CA: parity * 2 + (1 - c),
        W_CB: (1 - parity) * 2 + (1 - c),
    }

    stand_in = [
        pltpu.make_async_copy(k_in, kbuf.at[4], load_sem.at[8]),
        pltpu.make_async_copy(v_in, vbuf.at[4], load_sem.at[9]),
    ]
    stand_in_x = [
        pltpu.make_async_copy(k_in, kbuf.at[2], load_sem.at[10]),
        pltpu.make_async_copy(v_in, vbuf.at[2], load_sem.at[11]),
    ]
    first = z == 0
    first_two = (z * 2 + xl) == 0

    for j in range(NCH):
        @pl.when(z < 3)
        def _():
            kv_send(TO_Z, j, None)

        @pl.when(xl == 0)
        def _():
            kv_send(TO_X, j, None)

        @pl.when(c == 0)
        def _():
            kv_send(TO_C1, j, None)

        if j < NP:
            w_copy(W_CROSS, j, mine, from_input=True).start()


    @pl.when((xl == 1) & (z < 3))
    def _():
        for j in DIRECT:
            direct_send(j)

    load_k.start()
    load_v.start()

    def step_f(j):
        @pl.when(z > 0)
        def _():
            kv_wait(TO_Z, j)

        if j == 0:
            @pl.when(first)
            def _():
                for load in stand_in:
                    load.wait()

        if j not in DIRECT:
            @pl.when((xl == 1) & (z > 0))
            def _():
                kv_send(TO_X, j, 4)

        @pl.when(c == 1)
        def _():
            kv_send(TO_C3, j, 4)

    def step_g(j):
        @pl.when(z * 2 + xl > 0)
        def _():
            kv_wait(TO_X, j)

        if j == 0:
            @pl.when(first_two)
            def _():
                for load in stand_in_x:
                    load.wait()

        @pl.when(c == 0)
        def _():
            kv_send(TO_C3, j, 2)

        @pl.when(c == 1)
        def _():
            kv_send(TO_C1, j, 2)

    def step_e(j):
        kv_wait(TO_C1, j)
        kv_wait(TO_C3, j)

    def step_w(j):
        w_copy(W_CROSS, j, mine).wait_recv()
        w_copy(W_DOWN, j, mine).start()
        w_copy(W_CA, j, mine).start()

    def step_z(j):
        w_copy(W_DOWN, j, above).wait_recv()
        w_copy(W_CB, j, above).start()

    def norm_rows(i, carry):
        rows = pl.ds(pl.multiple_of(i * 16, 16), 16)
        x = hid[rows, :].astype(F32)
        r = lax.rsqrt(jnp.mean(x * x, axis=-1, keepdims=True) + 0.1)
        nrm[rows, :] = (x * r * gain[...].reshape(1, D)).astype(BF)
        return carry

    done = dict.fromkeys((step_f, step_g, step_e, step_w, step_z), 0)

    def upto(step, n):
        for j in range(done[step], n):
            step(j)
        done[step] = max(done[step], n)

    load_gain.wait()
    for slot in range(4):
        loads[slot].wait()
        lax.fori_loop(slot * 8, slot * 8 + 8, norm_rows, 0, unroll=4)
    @pl.when(first)
    def _():
        for load in stand_in:
            load.start()

    @pl.when(first_two)
    def _():
        for load in stand_in_x:
            load.start()

    load_wo.start()
    load_wq.wait()
    for slot in range(4):
        q = jnp.dot(nrm[slot * 128 : slot * 128 + 128, :], wq[...], preferred_element_type=F32)
        q = (q * SCALE).astype(BF)
        for kh in range(2):
            for g in range(2):
                head = 2 * kh + g
                qbuf[kh, slot * 256 + g * 128 : slot * 256 + g * 128 + 128, :] = q[
                    :, head * HD : head * HD + HD
                ]
        if slot == 1:
            upto(step_f, 1)
        if slot == 2:
            upto(step_f, 2)
    acc[...] = jnp.zeros_like(acc)
    for load in small:
        load.wait()
    load_k.wait()
    load_v.wait()

    off = starts[s] - s * CTX
    filled = {}
    for d in range(1, HALO + 1):
        source = s - d
        filled[d] = jnp.where(source >= 0, counts[jnp.maximum(source, 0)], 0)

    def attend(kh, tile, terms):
        lanes = slice(kh * HD, kh * HD + HD)
        rows = slice(tile * 512, tile * 512 + 512)
        q = qbuf[kh, rows, :]

        def scores(term):
            key = [kbuf[d, base : base + n, lanes] for d, base, n in term]
            key = key[0] if len(key) == 1 else jnp.concatenate(key, axis=0)
            return lax.dot_general(q, key, (((1,), (1,)), ((), ())), preferred_element_type=F32)

        def weights(x):
            return jnp.exp2(jnp.tanh(x * (1.0 / 50.0)) * EXP_SCALE)

        def values(term):
            out_rows = []
            for d, base, n in term:
                v = vbuf[d, base : base + n, lanes]
                if d == 0:
                    out_rows.append(jnp.concatenate([v, jnp.ones_like(v)], axis=1))
                else:
                    row_ids = lax.broadcasted_iota(jnp.int32, (n, HD), 0)
                    keep_row = jnp.where(row_ids < filled[d] - base, 1.0, 0.0).astype(BF)
                    out_rows.append(jnp.concatenate([v * keep_row, keep_row], axis=1))
            return out_rows[0] if len(out_rows) == 1 else jnp.concatenate(out_rows, axis=0)

        total = None
        for term in terms:
            if term[0][0] == 0:
                _, base, n = term[0]
                pattern = lax.broadcasted_iota(jnp.int32, (128, n), 1) - lax.broadcasted_iota(jnp.int32, (128, n), 0)
                near, far = scores(((0, base, n),)), scores(((4, base, n),))
                w_near, w_far = [], []
                for u in range(4):
                    limit = off + block_row((3, 1, 2, 0)[2 * tile + u // 2]) - base
                    is_near = pattern <= limit
                    part_rows = slice(u * 128, u * 128 + 128)
                    w = weights(jnp.where(is_near, near[part_rows], far[part_rows]))
                    w_near.append(jnp.where(is_near, w, 0.0).astype(BF))
                    w_far.append(jnp.where(is_near, 0.0, w).astype(BF))
                add = jnp.dot(
                    jnp.concatenate(w_near, axis=0), values(((0, base, n),)), preferred_element_type=F32
                )
                add = add + jnp.dot(
                    jnp.concatenate(w_far, axis=0), values(((4, base, n),)), preferred_element_type=F32
                )
            else:
                add = jnp.dot(weights(scores(term)).astype(BF), values(term), preferred_element_type=F32)
            total = add if total is None else total + add
        acc[kh, rows, :] += total

    def single(base, *distances):
        return tuple(((d, base, GR),) for d in distances)

    def units(tile, terms):
        for kh in range(2):
            attend(kh, tile, terms)

    LAST_A = (((1, 768, 128), (3, 768, 128)),)
    LAST_B = (((1, 896, 128), (3, 896, 128)),)

    upto(step_f, 5)
    upto(step_w, 1)
    upto(step_g, 2)
    upto(step_f, 6)
    upto(step_g, 3)
    upto(step_f, 7)
    upto(step_g, 4)
    upto(step_f, 8)
    upto(step_g, 5)
    upto(step_w, 2)
    upto(step_e, 1)
    units(0, single(0, 1, 2, 3, 0))
    upto(step_f, 10)
    upto(step_g, 6)
    units(1, single(0, 1, 2, 3, 0))
    upto(step_f, 11)
    upto(step_g, 8)
    upto(step_w, 3)
    upto(step_f, 12)
    upto(step_g, 9)
    upto(step_z, 1)
    upto(step_e, 2)
    units(0, single(256, 1, 2, 3, 0))
    upto(step_f, 14)
    upto(step_g, 11)
    upto(step_w, 4)
    units(1, single(256, 1, 2, 3, 0))
    upto(step_f, 15)
    upto(step_g, 12)
    upto(step_z, 2)
    upto(step_f, 16)
    upto(step_g, 13)
    upto(step_w, 5)
    upto(step_e, 3)
    units(0, single(512, 1, 2, 3, 0))
    upto(step_f, NCH)
    upto(step_g, 15)
    upto(step_z, 3)
    units(0, single(768, 0))
    upto(step_g, 16)
    upto(step_e, 4)
    units(0, LAST_A)
    upto(step_g, NCH)
    upto(step_w, 6)
    units(0, single(768, 2))
    upto(step_e, 5)

    def att_copy(slot, kh):
        rows = pl.ds(pl.multiple_of((1 - xh) * 64, 64), 64)
        cols = pl.ds(kh * 256, 256)
        return remote(
            att.at[slot, rows, cols], attr.at[slot, :, cols], att_s, att_r.at[slot, kh], x_far
        )

    def finish(kh, tile):
        a = acc[kh, tile * 512 : tile * 512 + 512, :]
        o = (a[:, :HD] / a[:, HD:]).astype(BF)
        for u in range(4):
            head = kh * 2 + u % 2
            att[2 * tile + u // 2, :, head * HD : head * HD + HD] = o[u * 128 : u * 128 + 128, :]
        for slot in (2 * tile, 2 * tile + 1):
            att_copy(slot, kh).start()

    attend(0, 0, LAST_B)
    finish(0, 0)
    attend(1, 0, LAST_B)
    finish(1, 0)
    upto(step_z, 4)
    units(1, single(512, 1, 2, 3, 0))
    units(1, single(768, 1, 2, 3, 0))
    upto(step_z, 5)
    finish(0, 1)
    finish(1, 1)

    def rs_copy(step, p):
        to = y_up if p < NP // 2 else y_down
        return remote(rs_s.at[step, p], rs_r.at[step, p], rss_sem.at[0 if p < NP // 2 else 1], rsr_sem.at[step, p], to)

    own_rows = pl.ds(pl.multiple_of(xh * 64, 64), 64)
    load_wo.wait()

    def own_part(tile, p):
        lhs = jnp.concatenate([att[2 * tile, own_rows, :], att[2 * tile + 1, own_rows, :]], axis=0)
        return jnp.dot(lhs, wo[:, p * PC : p * PC + PC], preferred_element_type=F32)

    def far_part(tile, p):
        lhs = jnp.concatenate([attr[2 * tile], attr[2 * tile + 1]], axis=0)
        return jnp.dot(lhs, wp[:, p * PC : p * PC + PC], preferred_element_type=F32)

    def att_arrived(tile):
        for slot in (2 * tile, 2 * tile + 1):
            for kh in range(2):
                att_copy(slot, kh).wait_recv()

    for p in PIECES:
        cols = slice(p * PC, p * PC + PC)
        r = own_part(0, p)
        part[0, :, cols] = r[:64]
        part[1, :, cols] = r[64:]
    att_arrived(0)
    for j, p in enumerate(PIECES):
        if j == 4:
            upto(step_z, 6)
        w_copy(W_CA, j, w_arrives[W_CA]).wait_recv()
        w_copy(W_CB, j, w_arrives[W_CB]).wait_recv()
        cols = slice(p * PC, p * PC + PC)
        r = far_part(0, p)
        first, later = (0, 1) if p < NP // 2 else (1, 0)
        rs_s[0, p] = (part[first, :, cols] + r[first * 64 : first * 64 + 64]).astype(BF)
        rs_copy(0, p).start()
        part[later, :, cols] += r[later * 64 : later * 64 + 64]
    att_arrived(1)
    for step in (1, 2):
        for p in PIECES:
            cols = slice(p * PC, p * PC + PC)
            if step == 1:
                r = own_part(1, p) + far_part(1, p)
                part[2, :, cols] = r[:64]
                part[3, :, cols] = r[64:]
            mine_slot = 2 if step == 1 else (1 if p < NP // 2 else 0)
            rs_copy(step - 1, p).wait_recv()
            rs_s[step, p] = (rs_r[step - 1, p].astype(F32) + part[mine_slot, :, cols]).astype(BF)
            rs_copy(step, p).start()
    squares = jnp.zeros((64, 1), F32)
    for p in PIECES:
        cols = slice(p * PC, p * PC + PC)
        rs_copy(2, p).wait_recv()
        whole = rs_r[2, p].astype(F32) + part[3, :, cols]
        part[3, :, cols] = whole
        squares = squares + jnp.sum(whole * whole, axis=-1, keepdims=True)
    factor = lax.rsqrt(squares * (1.0 / D) + 0.1)
    residual_rows = pl.ds(pl.multiple_of(384 + xh * 64, 64), 64)
    for p in range(NP):
        cols = slice(p * PC, p * PC + PC)
        residual = hid[residual_rows, cols].astype(F32)
        out[:, cols] = (residual + part[3, :, cols] * factor * post[cols].reshape(1, PC)).astype(BF)
    @pl.when(z < 3)
    def _():
        kv_sent(TO_Z)

    @pl.when(xl == 0)
    def _():
        kv_sent(TO_X)

    @pl.when((xl == 1) & (z > 0))
    def _():
        kv_sent(TO_X, CTX - DIRECT_ROWS)

    @pl.when((xl == 1) & (z < 3))
    def _():
        kv_sent(4, DIRECT_ROWS)

    for stream in (TO_C1, TO_C3):
        kv_sent(stream)
    for stream in (W_CROSS, W_DOWN, W_CA, W_CB):
        w_sent(stream)
    remote(attr, attr, att_s, att_r.at[0, 0], x_far).wait_send()
    half = rs_s.at[:, pl.ds(0, NP // 2)]
    remote(half, half, rss_sem.at[0], rsr_sem.at[0, 0], y_up).wait_send()
    remote(half, half, rss_sem.at[1], rsr_sem.at[0, 0], y_down).wait_send()


def shards(hidden_in, pre_gain, w_query, key_cache, value_cache, w_out, post_gain, starts, counts):
    hbm = pl.BlockSpec(memory_space=pltpu.HBM)
    dma = pltpu.SemaphoreType.DMA
    return pl.pallas_call(
        layer,
        out_shape=jax.ShapeDtypeStruct((64, D), BF),
        in_specs=[hbm] * 9,
        out_specs=pl.BlockSpec(memory_space=pltpu.VMEM),
        scratch_shapes=[
            pltpu.VMEM((D,), F32),
            pltpu.VMEM((D,), F32),
            pltpu.SMEM((16,), jnp.int32),
            pltpu.SMEM((16,), jnp.int32),
            pltpu.VMEM((QR, D), BF),
            pltpu.VMEM((QR, D), BF),
            pltpu.VMEM((D, 512), BF),
            pltpu.VMEM((HALO + 1, CTX, 256), BF),
            pltpu.VMEM((HALO + 1, CTX, 256), BF),
            pltpu.VMEM((2, 1024, HD), BF),
            pltpu.VMEM((2, 1024, 256), F32),
            pltpu.VMEM((4, 128, 512), BF),
            pltpu.VMEM((4, 64, 512), BF),
            pltpu.VMEM((512, D), BF),
            pltpu.VMEM((512, D), BF),
            pltpu.VMEM((4, 64, D), F32),
            pltpu.VMEM((3, NP, 64, PC), BF),
            pltpu.VMEM((3, NP, 64, PC), BF),
            dma((4,)),
            dma((12,)),
            dma((5,)),
            dma((2 * NCH + 2 * len(GROUPS),)),
            dma((4,)),
            dma((4, NP)),
            dma,
            dma((4, 2)),
            dma((2,)),
            dma((3, NP)),
        ],
        compiler_params=pltpu.CompilerParams(
            collective_id=0, has_side_effects=True, vmem_limit_bytes=50 * 1024 * 1024
        ),
        name="layer",
    )(
        *[
            pltpu.with_memory_space_constraint(x, pltpu.HBM)
            for x in (
                pre_gain, post_gain, starts, counts,
                hidden_in, w_query, key_cache, value_cache, w_out,
            )
        ]
    )


def solution(mesh):
    in_specs = (
        P("seq", None),
        P(),
        P(None, "tp"),
        P("seq", "tp"),
        P("seq", "tp"),
        P("tp", None),
        P(),
        P(),
        P(),
    )
    return jax.shard_map(
        shards, mesh=mesh, in_specs=in_specs, out_specs=P(("seq", "tp"), None), check_vma=False
    )
```
